32 devices in a mesh: hist: 8 (over y, x, core), col: 4 (over z).
Axes of the slice: x: 2, y: 2, z: 4, core: 2. Of those that a mesh axis runs over, the one named last changes fastest.
Arguments:
- less_row: bfloat16 [2, 128, 128, 1024], P(None, None, 'col', 'hist'), may hold values from -1.796875 to 1.796875
- less_col: bfloat16 [2, 128, 128, 1024], P(None, None, 'col', 'hist'), may hold values from -1.796875 to 1.796875
- great_row: bfloat16 [2, 128, 128, 1024], P(None, None, 'col', 'hist'), may hold values from -1.796875 to 1.796875
- great_col: bfloat16 [2, 128, 128, 1024], P(None, None, 'col', 'hist'), may hold values from -1.796875 to 1.796875
- density: float32 [2, 128, 128], replicated, may hold values from -1.8 to 1.8
- hamiltonian: float32 [128, 128], replicated, may hold values from -0.5 to 0.5
Outputs:
- less_row_out: bfloat16 [2, 128, 128, 1024], P(None, None, 'col', 'hist')
- less_col_out: bfloat16 [2, 128, 128, 1024], P(None, None, 'col', 'hist')
- great_row_out: bfloat16 [2, 128, 128, 1024], P(None, None, 'col', 'hist')
- great_col_out: bfloat16 [2, 128, 128, 1024], P(None, None, 'col', 'hist')
- density_out: float32 [2, 128, 128], replicated
The draws below stay inside these ranges and needn't reach their ends.
All inputs are finite; a program needn't handle non-finite values.
Results may differ from the reference program's by a relative error of at most 0.033.
Values may be sent and summed in bfloat16 or wider, within the bound.
No kernel may reach another device: no remote copies, remote signals or barrier semaphores. Data moves between devices by JAX's collectives and lax.ppermute only.
A program may use at most 128 MiB of HBM per device.

```python
import jax
import jax.numpy as jnp
from jax import lax

NORB = 128
STEPS = 3
HIST = 1024


def block_levels(own_key, shape, shards, smallest, top_value):
    gain, own = 1.0, jax.random.fold_in(own_key, 6)
    for position, shards_of in shards:
        heights = jnp.exp(jax.random.uniform(jax.random.fold_in(own, position), (shards_of,), jnp.float32, smallest / len(shards), top_value / len(shards)))
        gain = gain * jnp.repeat(heights, shape[position] // shards_of).reshape([-1 if axis == position else 1 for axis in range(len(shape))])
    return gain


def normal_values(rng, extent, width, bound, cuts=(), kind=jnp.bfloat16):
    entries = width * jax.random.normal(rng, extent, jnp.float32)
    if cuts:
        entries = entries * block_levels(rng, extent, cuts, -0.22, 0.18)
    return jnp.clip(entries, -bound, bound).astype(kind)


def setup_inputs(seed: int = 0) -> dict:
    seeds = jax.random.split(jax.random.key(seed), 7)
    less_row = normal_values(seeds[0], (2, NORB, NORB, HIST), 0.3, 1.796875, ((2, 4), (3, 8)))
    less_col = normal_values(seeds[1], (2, NORB, NORB, HIST), 0.3, 1.796875, ((2, 4), (3, 8)))
    great_row = normal_values(seeds[2], (2, NORB, NORB, HIST), 0.3, 1.796875, ((2, 4), (3, 8)))
    great_col = normal_values(seeds[3], (2, NORB, NORB, HIST), 0.3, 1.796875, ((2, 4), (3, 8)))
    density = normal_values(seeds[4], (2, NORB, NORB), 0.3, 1.8, (), jnp.float32)
    hamiltonian = normal_values(seeds[5], (NORB, NORB), NORB ** -0.5, 0.5, (), jnp.float32)
    return dict(less_row=less_row, less_col=less_col, great_row=great_row, great_col=great_col, density=density, hamiltonian=hamiltonian)


step_length = 0.1
mean_field = 2.0
coupling = 1.0

def unitary(hamiltonian, density):
    sym_ham = 0.5 * (hamiltonian + hamiltonian.T) + mean_field * jnp.diag(jnp.diagonal(density[0]))
    halved = 0.5 * step_length * sym_ham
    squared = jnp.dot(halved, halved, precision=lax.Precision.HIGHEST)
    identity = jnp.eye(sym_ham.shape[0], dtype=jnp.float32)
    factor = jnp.linalg.cholesky(identity + squared)
    unit_real = jax.scipy.linalg.cho_solve((factor, True), identity - squared)
    unit_imag = jax.scipy.linalg.cho_solve((factor, True), -2.0 * halved)
    return (unit_real, unit_imag)

def self_energy(row_hist, col_turned):
    green_real = row_hist[0].astype(jnp.float32)
    green_imag = row_hist[1].astype(jnp.float32)
    other_real = col_turned[0].astype(jnp.float32)
    other_imag = col_turned[1].astype(jnp.float32)
    square_real = green_real * green_real - green_imag * green_imag
    square_imag = 2.0 * green_real * green_imag
    out_real = coupling * coupling * (square_real * other_real - square_imag * other_imag)
    out_imag = coupling * coupling * (square_real * other_imag + square_imag * other_real)
    return jnp.stack([out_real, out_imag]).astype(jnp.bfloat16)

def contract_pair(first, second):
    return jnp.einsum('ikt,kjt->ij', first.astype(jnp.float32), second.astype(jnp.float32))

def contract(sigma, column):
    real_part = contract_pair(sigma[0], column[0]) - contract_pair(sigma[1], column[1])
    imag_part = contract_pair(sigma[0], column[1]) + contract_pair(sigma[1], column[0])
    return jnp.stack([real_part, imag_part])

def rotate_density(unit_real, unit_imag, rho):
    high = lax.Precision.HIGHEST
    left_real = jnp.dot(unit_real, rho[0], precision=high) - jnp.dot(unit_imag, rho[1], precision=high)
    left_imag = jnp.dot(unit_real, rho[1], precision=high) + jnp.dot(unit_imag, rho[0], precision=high)
    out_real = jnp.dot(left_real, unit_real.T, precision=high) + jnp.dot(left_imag, unit_imag.T, precision=high)
    out_imag = jnp.dot(left_imag, unit_real.T, precision=high) - jnp.dot(left_real, unit_imag.T, precision=high)
    return jnp.stack([out_real, out_imag])

def advance_rows(low_real, low_imag, history):
    count = history.shape[1]
    hist_real = history[0].reshape(count, -1)
    hist_imag = history[1].reshape(count, -1)
    out_real = jnp.dot(low_real.astype(jnp.float32), hist_real.astype(jnp.float32), preferred_element_type=jnp.float32) - jnp.dot(low_imag.astype(jnp.float32), hist_imag.astype(jnp.float32), preferred_element_type=jnp.float32)
    out_imag = jnp.dot(low_real.astype(jnp.float32), hist_imag.astype(jnp.float32), preferred_element_type=jnp.float32) + jnp.dot(low_imag.astype(jnp.float32), hist_real.astype(jnp.float32), preferred_element_type=jnp.float32)
    return jnp.stack([out_real, out_imag]).astype(jnp.bfloat16).reshape(history.shape)

def right_pair(first, matrix):
    return jnp.einsum('imt,jm->ijt', first.astype(jnp.float32), matrix.astype(jnp.float32))

def advance_cols(low_real, low_imag, history):
    out_real = right_pair(history[0], low_real) + right_pair(history[1], low_imag)
    out_imag = right_pair(history[1], low_real) - right_pair(history[0], low_imag)
    return jnp.stack([out_real, out_imag]).astype(jnp.bfloat16)

def reference(less_row, less_col, great_row, great_col, density, hamiltonian):
    rho = density
    for step_index in range(STEPS):
        unit_real, unit_imag = unitary(hamiltonian, rho)
        sigma_less = self_energy(less_row, jnp.swapaxes(great_col, 1, 2))
        sigma_great = self_energy(great_row, jnp.swapaxes(less_col, 1, 2))
        collision = step_length * (contract(sigma_great, less_col) - contract(sigma_less, great_col))
        rho = rotate_density(unit_real, unit_imag, rho) + collision
        low_real = unit_real.astype(jnp.bfloat16)
        low_imag = unit_imag.astype(jnp.bfloat16)
        less_row = advance_rows(low_real, low_imag, less_row)
        great_row = advance_rows(low_real, low_imag, great_row)
        less_col = advance_cols(low_real, low_imag, less_col)
        great_col = advance_cols(low_real, low_imag, great_col)
    return (less_row, less_col, great_row, great_col, rho)
```

```python
import jax
import jax.numpy as jnp
from jax import lax
from jax.sharding import PartitionSpec as P

STEPS = 3


step_length = 0.1
mean_field = 2.0
coupling = 1.0


def unitary(hamiltonian, level):
    sym_ham = 0.5 * (hamiltonian + hamiltonian.T) + mean_field * jnp.diag(level)
    halved = 0.5 * step_length * sym_ham
    squared = jnp.dot(halved, halved, precision=lax.Precision.HIGHEST)
    identity = jnp.eye(sym_ham.shape[0], dtype=jnp.float32)
    factor = jnp.linalg.cholesky(identity + squared)
    unit_real = jax.scipy.linalg.cho_solve((factor, True), identity - squared)
    unit_imag = jax.scipy.linalg.cho_solve((factor, True), -2.0 * halved)
    return (unit_real, unit_imag)


def self_energy(row_hist, col_turned):
    green_real = row_hist[0].astype(jnp.float32)
    green_imag = row_hist[1].astype(jnp.float32)
    other_real = col_turned[0].astype(jnp.float32)
    other_imag = col_turned[1].astype(jnp.float32)
    square_real = green_real * green_real - green_imag * green_imag
    square_imag = 2.0 * green_real * green_imag
    out_real = coupling * coupling * (square_real * other_real - square_imag * other_imag)
    out_imag = coupling * coupling * (square_real * other_imag + square_imag * other_real)
    return jnp.stack([out_real, out_imag]).astype(jnp.bfloat16)


def contract_pair(first, second):
    return jnp.einsum("ikt,kjt->ij", first, second, preferred_element_type=jnp.float32)


def contract(sigma, rows_block):
    real_part = contract_pair(sigma[0], rows_block[0]) - contract_pair(sigma[1], rows_block[1])
    imag_part = contract_pair(sigma[0], rows_block[1]) + contract_pair(sigma[1], rows_block[0])
    return jnp.stack([real_part, imag_part])


def rotate_density(unit_real, unit_imag, rho):
    high = lax.Precision.HIGHEST
    left_real = jnp.dot(unit_real, rho[0], precision=high) - jnp.dot(
        unit_imag, rho[1], precision=high
    )
    left_imag = jnp.dot(unit_real, rho[1], precision=high) + jnp.dot(
        unit_imag, rho[0], precision=high
    )
    out_real = jnp.dot(left_real, unit_real.T, precision=high) + jnp.dot(
        left_imag, unit_imag.T, precision=high
    )
    out_imag = jnp.dot(left_imag, unit_real.T, precision=high) - jnp.dot(
        left_real, unit_imag.T, precision=high
    )
    return jnp.stack([out_real, out_imag])


def advance_rows(low_real, low_imag, history):
    count = history.shape[1]
    hist_real = history[0].reshape(count, -1)
    hist_imag = history[1].reshape(count, -1)
    out_real = jnp.dot(low_real, hist_real, preferred_element_type=jnp.float32) - jnp.dot(
        low_imag, hist_imag, preferred_element_type=jnp.float32
    )
    out_imag = jnp.dot(low_real, hist_imag, preferred_element_type=jnp.float32) + jnp.dot(
        low_imag, hist_real, preferred_element_type=jnp.float32
    )
    return jnp.stack([out_real, out_imag]).astype(jnp.bfloat16).reshape(history.shape)


def right_pair(first, matrix):
    return jnp.einsum("imt,jm->ijt", first, matrix, preferred_element_type=jnp.float32)


def advance_cols(low_real, low_imag, rows_block):
    out_real = right_pair(rows_block[0], low_real) + right_pair(rows_block[1], low_imag)
    out_imag = right_pair(rows_block[1], low_real) - right_pair(rows_block[0], low_imag)
    return jnp.stack([out_real, out_imag]).astype(jnp.bfloat16)


def axis_total(values, name):
    size = lax.axis_size(name)
    distance = 1
    while distance < size:
        values = values + lax.ppermute(values, name, [(j, j ^ distance) for j in range(size)])
        distance *= 2
    return values


def total(values):
    return axis_total(axis_total(values, "hist"), "col")


def row_total(row):
    axes = ("hist", "col")
    count = lax.axis_size("hist") * lax.axis_size("col")
    spread = lax.all_to_all(jnp.broadcast_to(row, (count,) + row.shape), axes, 0, 0, tiled=True)
    return jnp.sum(spread, axis=0)


def diagonal_of(matrix):
    size = matrix.shape[0]
    keep = lax.broadcasted_iota(jnp.int32, (size, size), 0) == lax.broadcasted_iota(jnp.int32, (size, size), 1)
    return jnp.sum(jnp.where(keep, matrix, 0.0), axis=0)


def per_device(less_row, less_col, great_row, great_col, density, hamiltonian):
    rows_great = lax.all_to_all(great_col, "col", split_axis=1, concat_axis=2, tiled=True)
    rows_less = lax.all_to_all(less_col, "col", split_axis=1, concat_axis=2, tiled=True)

    def partial_collision(less_row, great_row, rows_less, rows_great):
        sigma_less = self_energy(less_row, jnp.swapaxes(rows_great, 1, 2))
        sigma_great = self_energy(great_row, jnp.swapaxes(rows_less, 1, 2))
        return step_length * (contract(sigma_great, rows_less) - contract(sigma_less, rows_great))

    def advance(unit, less_row, great_row, rows_less, rows_great):
        low_real, low_imag = unit[0].astype(jnp.bfloat16), unit[1].astype(jnp.bfloat16)
        return (
            advance_rows(low_real, low_imag, less_row),
            advance_rows(low_real, low_imag, great_row),
            advance_cols(low_real, low_imag, rows_less),
            advance_cols(low_real, low_imag, rows_great),
        )

    histories = (less_row, great_row, rows_less, rows_great)
    known, pending = density, None
    level = diagonal_of(density[0])
    for step_index in range(STEPS):
        unit = unitary(hamiltonian, level)
        partial_sum = partial_collision(*histories)
        histories = advance(unit, *histories)
        known = rotate_density(*unit, known)
        pending = partial_sum if pending is None else rotate_density(*unit, pending) + partial_sum
        if step_index < STEPS - 1:
            level = diagonal_of(known[0]) + row_total(diagonal_of(pending[0]))
    less_row, great_row, rows_less, rows_great = histories
    great_col = lax.all_to_all(rows_great, "col", split_axis=2, concat_axis=1, tiled=True)
    less_col = lax.all_to_all(rows_less, "col", split_axis=2, concat_axis=1, tiled=True)
    return (less_row, less_col, great_row, great_col, known + total(pending))


def solution(mesh):
    in_specs = (
        P(None, None, "col", "hist"),
        P(None, None, "col", "hist"),
        P(None, None, "col", "hist"),
        P(None, None, "col", "hist"),
        P(),
        P(),
    )
    out_specs = (
        P(None, None, "col", "hist"),
        P(None, None, "col", "hist"),
        P(None, None, "col", "hist"),
        P(None, None, "col", "hist"),
        P(),
    )
    return jax.shard_map(
        per_device, mesh=mesh, in_specs=in_specs, out_specs=out_specs, check_vma=False
    )
```

```python
import functools

import jax
import jax.numpy as jnp
from jax import lax
from jax.experimental import pallas as pl
from jax.experimental.pallas import tpu as pltpu
from jax.sharding import PartitionSpec as P


STEPS = 3

step_length = 0.1
mean_field = 2.0
coupling = 1.0

HIGH = lax.Precision.HIGHEST
SUBLANES = 8
GROUP = 8
SPAN = 256


def dot_high(a, b):
    return jnp.dot(a, b, precision=HIGH, preferred_element_type=jnp.float32)


def eye_mask(size):
    rows = lax.broadcasted_iota(jnp.int32, (size, size), 0)
    return rows == lax.broadcasted_iota(jnp.int32, (size, size), 1)


def inverse(matrix):
    size = matrix.shape[0]
    blocks = [matrix[p : p + SUBLANES] for p in range(0, size, SUBLANES)]
    rows = lax.broadcasted_iota(jnp.int32, (SUBLANES, size), 0)
    lanes = lax.broadcasted_iota(jnp.int32, (SUBLANES, size), 1)
    for p in range(len(blocks)):
        first = p * SUBLANES
        pivot_lanes = (lanes >= first) & (lanes < first + SUBLANES)

        def columns(block):
            return [jnp.broadcast_to(block[:, first + c : first + c + 1], (SUBLANES, size)) for c in range(SUBLANES)]

        pivot = columns(blocks[p])
        row_block = jnp.where(pivot_lanes, jnp.where(lanes == rows + first, 1.0, 0.0), blocks[p])
        for j in range(SUBLANES):

            def across(value):
                return jnp.broadcast_to(value[j : j + 1], (SUBLANES, size))

            scale = 1.0 / across(pivot[j])
            factor = pivot[j]

            def eliminate(value):
                top = across(value) * scale
                return jnp.where(rows == j, top, value - factor * top)

            row_block = eliminate(row_block)
            pivot = [eliminate(value) if c > j else value for c, value in enumerate(pivot)]
        spread = [jnp.broadcast_to(row_block[c : c + 1], (SUBLANES, size)) for c in range(SUBLANES)]
        order = list(range(p + 1, len(blocks))) + list(range(p))
        for q in order:
            total = jnp.where(pivot_lanes, 0.0, blocks[q])
            for c, column in enumerate(columns(blocks[q])):
                total = total - column * spread[c]
            blocks[q] = total
        blocks[p] = row_block
    return jnp.concatenate(blocks, axis=0)


def solve_kernel(levels_ref, ham_ref, rho_ref, low_ref, left_ref, unit_ref, diag_ref):
    size = ham_ref.shape[0]
    eye = eye_mask(size)
    level = jnp.sum(levels_ref[...], axis=0, keepdims=True)
    halved = (0.5 * step_length) * (ham_ref[...] + mean_field * jnp.where(eye, level, 0.0))
    identity = jnp.where(eye, 1.0, 0.0)
    solved = inverse(identity + dot_high(halved, halved))
    unit_real = 2.0 * solved - identity
    unit_imag = -2.0 * dot_high(solved, halved)
    low_real, low_imag = unit_real.astype(jnp.bfloat16), unit_imag.astype(jnp.bfloat16)
    low_ref[0:size, 0:size] = low_real
    low_ref[0:size, size:] = low_imag
    low_ref[size:, 0:size] = -low_imag
    low_ref[size:, size:] = low_real
    unit_ref[0] = unit_real
    unit_ref[1] = unit_imag
    rho_real, rho_imag = rho_ref[0], rho_ref[1]
    left_real = dot_high(unit_real, rho_real) - dot_high(unit_imag, rho_imag)
    left_imag = dot_high(unit_real, rho_imag) + dot_high(unit_imag, rho_real)
    left_ref[0] = left_real
    left_ref[1] = left_imag
    real_diagonal = jnp.sum(left_real * unit_real + left_imag * unit_imag, axis=1, keepdims=True)
    diag_ref[...] = jnp.sum(jnp.where(eye, real_diagonal, 0.0), axis=0, keepdims=True)


def solve(levels, hamiltonian, rho):
    size = hamiltonian.shape[0]
    f32 = jnp.float32
    return pl.pallas_call(
        solve_kernel,
        out_shape=(
            jax.ShapeDtypeStruct((2 * size, 2 * size), jnp.bfloat16),
            jax.ShapeDtypeStruct((2, size, size), f32),
            jax.ShapeDtypeStruct((2, size, size), f32),
            jax.ShapeDtypeStruct((1, size), f32),
        ),
        cost_estimate=pl.CostEstimate(flops=40_000_000, bytes_accessed=1_000_000, transcendentals=0),
        name="solve",
    )(levels, hamiltonian, rho)


def sigma_into(sig_ref, row_ref, col_ref, rows, span):
    size = sig_ref.shape[0] // 2
    for start in range(0, size, rows):
        for first in range(0, sig_ref.shape[1], span):
            real, imag = pl.ds(start, rows), pl.ds(size + start, rows)
            lanes = pl.ds(first, span)
            green_real = row_ref[real, lanes].astype(jnp.float32)
            green_imag = row_ref[imag, lanes].astype(jnp.float32)
            other_real = col_ref[real, lanes].astype(jnp.float32)
            other_imag = col_ref[imag, lanes].astype(jnp.float32)
            square_real = (coupling * coupling) * (green_real * green_real - green_imag * green_imag)
            square_imag = (coupling * coupling * 2.0) * green_real * green_imag
            sig_ref[real, lanes] = (square_real * other_real - square_imag * other_imag).astype(jnp.bfloat16)
            sig_ref[imag, lanes] = (square_real * other_imag + square_imag * other_real).astype(jnp.bfloat16)


def overlap(sig, col):
    return lax.dot_general(sig, col, (((1,), (1,)), ((), ())), preferred_element_type=jnp.float32)


def advance_into(out_ref, low, source_ref, span):
    for first in range(0, source_ref.shape[1], span):
        lanes = pl.ds(first, span)
        source = source_ref[:, lanes].astype(jnp.bfloat16)
        out_ref[:, lanes] = jnp.dot(low, source, preferred_element_type=jnp.float32).astype(out_ref.dtype)


def row_form(low):
    size = low.shape[0] // 2
    top = jnp.concatenate([low[:size, :size], low[size:, :size]], axis=1)
    bottom = jnp.concatenate([low[:size, size:], low[:size, :size]], axis=1)
    return jnp.concatenate([top, bottom], axis=0)


def accumulate(ref, value):
    @pl.when(pl.program_id(0) == 0)
    def _():
        ref[...] = value

    @pl.when(pl.program_id(0) != 0)
    def _():
        ref[...] += value


def first_kernel(parts, me_ref, row_ref, later_row_ref, *refs):
    pieces, (low_ref, now_ref, later_ref, col_out, place, sig) = refs[:parts], refs[parts:]
    _, group, block, times = pieces[0].shape
    size = place.shape[0] // 2
    for r in range(parts):
        source = lax.rem(me_ref[0] + r, parts) * block
        for part in range(2):
            rows = pl.ds(pl.multiple_of(part * size + source, block), block)
            for k in range(group):
                place[rows, pl.ds(k * times, times)] = pieces[r][part, k].astype(place.dtype)
    sigma_into(sig, row_ref, place, 16, SPAN)
    accumulate(now_ref, overlap(sig[...], place[...].astype(jnp.bfloat16)))
    advance_into(col_out, low_ref[...], place, SPAN)
    sigma_into(sig, later_row_ref, col_out, 16, SPAN)
    accumulate(later_ref, overlap(sig[...], col_out[...]))


def middle_kernel(row_ref, col_ref, low_ref, sum_ref, row_out, col_out, sig):
    low = low_ref[...]
    advance_into(row_out, row_form(low), row_ref, SPAN)
    advance_into(col_out, low, col_ref, SPAN)
    sigma_into(sig, row_out, col_out, 16, SPAN)
    accumulate(sum_ref, overlap(sig[...], col_out[...]))


def row_kernel(row_ref, low_ref, row_out):
    advance_into(row_out, row_form(low_ref[...]), row_ref, SPAN)


def last_kernel(parts, me_ref, col_ref, low_ref, *refs):
    outs, moved = refs[:parts], refs[parts]
    _, group, block, times = outs[0].shape
    size = moved.shape[0] // 2
    advance_into(moved, low_ref[...], col_ref, SPAN)
    for r in range(parts):
        target = lax.rem(me_ref[0] + r, parts) * block
        for part in range(2):
            rows = pl.ds(pl.multiple_of(part * size + target, block), block)
            for k in range(group):
                outs[r][part, k] = moved[rows, pl.ds(k * times, times)].astype(jnp.bfloat16)


def whole(shape):
    return pl.BlockSpec(shape, lambda g, *_: (0,) * len(shape))


def history_spec(size, width):
    return pl.BlockSpec((2 * size, width), lambda g, *_: (0, g))


def cost(arrays, products):
    return pl.CostEstimate(flops=products * 2 * 256 * 256 * 4096, bytes_accessed=arrays * 2**21, transcendentals=0)


def place_type(block):
    return jnp.bfloat16 if block % 16 == 0 else jnp.float32


def first_steps(me, row, later_row, own, pieces, low):
    size = own.shape[1]
    _, count, block, times = pieces[0].shape
    parts = len(pieces) + 1
    group = min(GROUP, count)
    width = group * times
    groups = count // group
    piece = pl.BlockSpec((2, group, block, times), lambda g, me: (0, g, 0, 0))
    mine = pl.BlockSpec((2, group, block, times), lambda g, me: (0, me[0] * groups + g, 0, 0))
    square = jax.ShapeDtypeStruct((2 * size, 2 * size), jnp.float32)
    return pl.pallas_call(
        functools.partial(first_kernel, parts),
        grid_spec=pltpu.PrefetchScalarGridSpec(
            num_scalar_prefetch=1,
            grid=(groups,),
            in_specs=[history_spec(size, width)] * 2
            + [mine]
            + [piece] * len(pieces)
            + [whole((2 * size, 2 * size))],
            out_specs=[whole((2 * size, 2 * size))] * 2 + [history_spec(size, width)],
            scratch_shapes=[
                pltpu.VMEM((2 * size, width), place_type(block)),
                pltpu.VMEM((2 * size, width), jnp.bfloat16),
            ],
        ),
        out_shape=[square, square, jax.ShapeDtypeStruct(row.shape, jnp.bfloat16)],
        cost_estimate=cost(4, 3),
        name="first_steps",
    )(me, row, later_row, own, *pieces, low)


def middle_step(row, col, low, width):
    double = row.shape[0]
    size = double // 2
    return pl.pallas_call(
        middle_kernel,
        grid=(row.shape[1] // width,),
        in_specs=[history_spec(size, width)] * 2 + [whole((double, double))],
        out_specs=[whole((double, double))] + [history_spec(size, width)] * 2,
        scratch_shapes=[pltpu.VMEM((double, width), jnp.bfloat16)],
        out_shape=[
            jax.ShapeDtypeStruct((double, double), jnp.float32),
            jax.ShapeDtypeStruct(row.shape, jnp.bfloat16),
            jax.ShapeDtypeStruct(row.shape, jnp.bfloat16),
        ],
        cost_estimate=cost(4, 3),
        name="middle_step",
    )(row, col, low)


def row_step(row, low, width):
    double = row.shape[0]
    return pl.pallas_call(
        row_kernel,
        grid=(row.shape[1] // width,),
        in_specs=[history_spec(double // 2, width), whole((double, double))],
        out_specs=history_spec(double // 2, width),
        out_shape=jax.ShapeDtypeStruct(row.shape, jnp.bfloat16),
        cost_estimate=cost(2, 1),
        name="row_step",
    )(row, low)


def last_step(me, col, low, parts, count, times):
    double = col.shape[0]
    block = double // 2 // parts
    group = min(GROUP, count)
    width = group * times
    piece = pl.BlockSpec((2, group, block, times), lambda g, me: (0, g, 0, 0))
    return pl.pallas_call(
        functools.partial(last_kernel, parts),
        grid_spec=pltpu.PrefetchScalarGridSpec(
            num_scalar_prefetch=1,
            grid=(count // group,),
            in_specs=[history_spec(double // 2, width), whole((double, double))],
            out_specs=[piece] * parts,
            scratch_shapes=[pltpu.VMEM((double, width), place_type(block))],
        ),
        out_shape=[jax.ShapeDtypeStruct((2, count, block, times), jnp.bfloat16)] * parts,
        cost_estimate=cost(2, 1),
        name="last_step",
    )(me, col, low)


def axis_total(values, name):
    size = lax.axis_size(name)
    distance = 1
    while distance < size:
        values = values + lax.ppermute(values, name, [(j, j ^ distance) for j in range(size)])
        distance *= 2
    return values


def total(values):
    return axis_total(axis_total(values, "hist"), "col")


def all_rows(row):
    count = lax.axis_size("hist") * lax.axis_size("col")
    spread = jnp.broadcast_to(row.reshape(1, -1), (count, row.size))
    return lax.all_to_all(spread, ("hist", "col"), 0, 0, tiled=True)


def diagonal_of(matrix):
    return jnp.sum(jnp.where(eye_mask(matrix.shape[0]), matrix, 0.0), axis=0, keepdims=True)


def collision_of(plus, minus):
    both = step_length * (plus - minus)
    size = both.shape[0] // 2
    return jnp.stack([both[:size, :size] - both[size:, size:], both[:size, size:] + both[size:, :size]])


def finish_rotation(left, unit):
    high = functools.partial(jnp.dot, precision=HIGH)
    real = high(left[0], unit[0].T) + high(left[1], unit[1].T)
    imag = high(left[1], unit[0].T) - high(left[0], unit[1].T)
    return jnp.stack([real, imag])


def gather_pieces(col):
    me, parts = lax.axis_index("col"), lax.axis_size("col")
    count = col.shape[1] // parts
    pieces = []
    for r in range(1, parts):
        target = lax.rem(me + (parts - r), parts)
        piece = lax.dynamic_slice_in_dim(col, target * count, count, axis=1)
        pieces.append(lax.ppermute(piece, "col", [(j, (j - r) % parts) for j in range(parts)]))
    return pieces


def return_pieces(pieces):
    me, parts = lax.axis_index("col"), lax.axis_size("col")
    _, count, block, times = pieces[0].shape
    out = jnp.zeros((2, parts * count, block, times), pieces[0].dtype)
    for r, piece in enumerate(pieces):
        moved = piece if r == 0 else lax.ppermute(piece, "col", [(j, (j + r) % parts) for j in range(parts)])
        source = lax.rem(me + (parts - r), parts)
        out = lax.dynamic_update_slice_in_dim(out, moved, source * count, axis=1)
    return out


def per_device(less_row, less_col, great_row, great_col, density, hamiltonian):
    size, count, times = less_row.shape[1:]
    parts = lax.axis_size("col")
    devices = parts * lax.axis_size("hist")
    me = lax.axis_index("col").astype(jnp.int32).reshape(1)
    width = min(GROUP, count) * times

    great_pieces = gather_pieces(great_col)
    less_pieces = gather_pieces(less_col)

    symmetric = 0.5 * (hamiltonian + hamiltonian.T)
    share = density * (1.0 / devices)
    low, left, unit, level = solve(diagonal_of(density[0]), symmetric, share)
    rho = finish_rotation(left, unit)

    less = less_row.reshape(2 * size, count * times)
    great = great_row.reshape(2 * size, count * times)
    less_next = row_step(less, low, width)
    great_next = row_step(great, low, width)
    minus_now, minus_later, cols_great = first_steps(me, less, less_next, great_col, great_pieces, low)
    plus_now, plus_later, cols_less = first_steps(me, great, great_next, less_col, less_pieces, low)

    rho = rho + collision_of(plus_now, minus_now)
    levels = all_rows(diagonal_of(rho[0]))
    low, left, unit, level = solve(levels, symmetric, rho)
    later = collision_of(plus_later, minus_later)
    levels = all_rows(level + diagonal_of(later[0]))
    minus, less_next, cols_great = middle_step(less_next, cols_great, low, width)
    plus, great_next, cols_less = middle_step(great_next, cols_less, low, width)
    rho = finish_rotation(left, unit) + later

    low, left, unit, level = solve(levels, symmetric, rho)
    great_out = return_pieces(last_step(me, cols_great, low, parts, count, times))
    less_out = return_pieces(last_step(me, cols_less, low, parts, count, times))
    rho = total(finish_rotation(left, unit) + collision_of(plus, minus))
    less_row_out = row_step(less_next, low, width).reshape(less_row.shape)
    great_row_out = row_step(great_next, low, width).reshape(great_row.shape)
    return (less_row_out, less_out, great_row_out, great_out, rho)


def solution(mesh):
    history = P(None, None, "col", "hist")
    return jax.shard_map(
        per_device,
        mesh=mesh,
        in_specs=(history, history, history, history, P(), P()),
        out_specs=(history, history, history, history, P()),
        check_vma=False,
    )
```

```python
import functools

import jax
import jax.numpy as jnp
from jax import lax
from jax.experimental import pallas as pl
from jax.experimental.pallas import tpu as pltpu
from jax.sharding import PartitionSpec as P


STEPS = 3

step_length = 0.1
mean_field = 2.0
coupling = 1.0

HIGH = lax.Precision.HIGHEST
SUBLANES = 8
GROUP = 8
SPAN = 256


def dot_high(a, b):
    return jnp.dot(a, b, precision=HIGH, preferred_element_type=jnp.float32)


def eye_mask(size):
    rows = lax.broadcasted_iota(jnp.int32, (size, size), 0)
    return rows == lax.broadcasted_iota(jnp.int32, (size, size), 1)


def inverse(matrix):
    size = matrix.shape[0]
    blocks = [matrix[p : p + SUBLANES] for p in range(0, size, SUBLANES)]
    rows = lax.broadcasted_iota(jnp.int32, (SUBLANES, size), 0)
    lanes = lax.broadcasted_iota(jnp.int32, (SUBLANES, size), 1)
    for p in range(len(blocks)):
        first = p * SUBLANES
        pivot_lanes = (lanes >= first) & (lanes < first + SUBLANES)

        def columns(block):
            return [jnp.broadcast_to(block[:, first + c : first + c + 1], (SUBLANES, size)) for c in range(SUBLANES)]

        pivot = columns(blocks[p])
        row_block = jnp.where(pivot_lanes, jnp.where(lanes == rows + first, 1.0, 0.0), blocks[p])
        for j in range(SUBLANES):

            def across(value):
                return jnp.broadcast_to(value[j : j + 1], (SUBLANES, size))

            scale = 1.0 / across(pivot[j])
            factor = pivot[j]

            def eliminate(value):
                top = across(value) * scale
                return jnp.where(rows == j, top, value - factor * top)

            row_block = eliminate(row_block)
            pivot = [eliminate(value) if c > j else value for c, value in enumerate(pivot)]
        spread = [jnp.broadcast_to(row_block[c : c + 1], (SUBLANES, size)) for c in range(SUBLANES)]
        order = list(range(p + 1, len(blocks))) + list(range(p))
        for q in order:
            total = jnp.where(pivot_lanes, 0.0, blocks[q])
            for c, column in enumerate(columns(blocks[q])):
                total = total - column * spread[c]
            blocks[q] = total
        blocks[p] = row_block
    return jnp.concatenate(blocks, axis=0)


def spread_rows(ref, row):
    ref[...] = jnp.broadcast_to(row.reshape(1, 1, row.shape[-1]), ref.shape)


def diagonal_row(matrix):
    return jnp.sum(jnp.where(eye_mask(matrix.shape[0]), matrix, 0.0), axis=0, keepdims=True)


def solve_kernel(rotates, levels_ref, ham_ref, *refs):
    size = ham_ref.shape[0]
    eye = eye_mask(size)
    level = levels_ref[0]
    for row in range(1, levels_ref.shape[0]):
        level = level + levels_ref[row]
    halved = (0.5 * step_length) * (ham_ref[...] + mean_field * jnp.where(eye, level, 0.0))
    identity = jnp.where(eye, 1.0, 0.0)
    solved = inverse(identity + dot_high(halved, halved))
    unit_real = 2.0 * solved - identity
    unit_imag = -2.0 * dot_high(solved, halved)
    low_real, low_imag = unit_real.astype(jnp.bfloat16), unit_imag.astype(jnp.bfloat16)
    if rotates:
        rho_ref, later_ref, low_ref, unit_ref, left_ref, next_ref = refs
    else:
        low_ref, unit_ref = refs
    low_ref[0:size, 0:size] = low_real
    low_ref[0:size, size:] = low_imag
    low_ref[size:, 0:size] = -low_imag
    low_ref[size:, size:] = low_real
    unit_ref[0] = unit_real
    unit_ref[1] = unit_imag
    if rotates:
        rho_real, rho_imag = rho_ref[0], rho_ref[1]
        left_real = dot_high(unit_real, rho_real) - dot_high(unit_imag, rho_imag)
        left_imag = dot_high(unit_real, rho_imag) + dot_high(unit_imag, rho_real)
        left_ref[0] = left_real
        left_ref[1] = left_imag
        real_diagonal = jnp.sum(left_real * unit_real + left_imag * unit_imag, axis=1, keepdims=True)
        row = jnp.sum(jnp.where(eye, real_diagonal + later_ref[0], 0.0), axis=0, keepdims=True)
        spread_rows(next_ref, row)


IN_VMEM = pl.BlockSpec(memory_space=pltpu.VMEM)
GRANT = pltpu.CompilerParams(vmem_limit_bytes=8 * 2**20)


def call(body, outs, args, cost_estimate, name, scratch=(), scalars=0):
    specs = [pl.BlockSpec(memory_space=pltpu.SMEM)] * scalars + [IN_VMEM] * (len(args) - scalars)
    return pl.pallas_call(
        body,
        out_shape=[jax.ShapeDtypeStruct(shape, kind) for shape, kind in outs],
        in_specs=specs,
        out_specs=[IN_VMEM] * len(outs),
        scratch_shapes=list(scratch),
        cost_estimate=cost_estimate,
        compiler_params=GRANT,
        name=name,
    )(*args)


def solve(levels, hamiltonian, rho=None, later=None):
    size = hamiltonian.shape[0]
    outs = [((2 * size, 2 * size), jnp.bfloat16), ((2, size, size), jnp.float32)]
    args = (levels, hamiltonian)
    if rho is not None:
        outs += [((2, size, size), jnp.float32), (levels.shape, jnp.float32)]
        args += (rho, later)
    estimate = pl.CostEstimate(flops=4_000_000_000, bytes_accessed=1_000_000, transcendentals=0)
    return call(functools.partial(solve_kernel, rho is not None), outs, args, estimate, "solve")


def lanes_of(base, first, span):
    return pl.ds(pl.multiple_of(base + first, 128), span)


def sigma_into(sig_ref, row_ref, col_ref, base, rows, span):
    size = sig_ref.shape[0] // 2
    for start in range(0, size, rows):
        for first in range(0, sig_ref.shape[1], span):
            real, imag = pl.ds(start, rows), pl.ds(size + start, rows)
            lanes, here = lanes_of(base, first, span), pl.ds(first, span)
            green_real = row_ref[real, lanes].astype(jnp.float32)
            green_imag = row_ref[imag, lanes].astype(jnp.float32)
            other_real = col_ref[real, lanes].astype(jnp.float32)
            other_imag = col_ref[imag, lanes].astype(jnp.float32)
            square_real = (coupling * coupling) * (green_real * green_real - green_imag * green_imag)
            square_imag = (coupling * coupling * 2.0) * green_real * green_imag
            sig_ref[real, here] = (square_real * other_real - square_imag * other_imag).astype(jnp.bfloat16)
            sig_ref[imag, here] = (square_real * other_imag + square_imag * other_real).astype(jnp.bfloat16)


def overlap(sig, col):
    return lax.dot_general(sig, col, (((1,), (1,)), ((), ())), preferred_element_type=jnp.float32)


def advance_into(out_ref, low, source_ref, base, width, local=False):
    span = min(SPAN, width)
    for first in range(0, width, span):
        lanes = lanes_of(base, first, span)
        target = pl.ds(first, span) if local else lanes
        moved = jnp.dot(low, source_ref[:, lanes], preferred_element_type=jnp.float32)
        out_ref[:, target] = moved.astype(out_ref.dtype)


def row_form(low):
    size = low.shape[0] // 2
    top = jnp.concatenate([low[:size, :size], low[size:, :size]], axis=1)
    bottom = jnp.concatenate([low[:size, size:], low[:size, :size]], axis=1)
    return jnp.concatenate([top, bottom], axis=0)


def each_group(total_width, width, body):
    def step(g, carry):
        body(pl.multiple_of(g * width, width))
        return carry

    lax.fori_loop(0, total_width // width, step, 0)


def complex_sum(four):
    size = four.shape[0] // 2
    return four[:size, :size] - four[size:, size:], four[:size, size:] + four[size:, :size]


def finish_sum(acc, before_ref, base_ref, out_ref, scale):
    real, imag = complex_sum(scale * (acc[...] - before_ref[...]))
    if base_ref is not None:
        real, imag = base_ref[0] + real, base_ref[1] + imag
    out_ref[0] = real
    out_ref[1] = imag
    return real


def now_kernel(parts, last, me_ref, row_ref, own_ref, *refs):
    pieces, refs = refs[: parts - 1], refs[parts - 1 :]
    if last:
        before_ref, known_ref, col_out, rho_out, level_out, acc, sig, place = refs
    else:
        col_out, acc, sig, place = refs
    _, count, block, times = pieces[0].shape
    width = sig.shape[1]
    group = width // times
    size = sig.shape[0] // 2
    direct = place.dtype == col_out.dtype
    acc[...] = jnp.zeros_like(acc)

    def body(base):
        first = lax.div(base, times)
        for r in range(parts):
            source = lax.bitwise_xor(me_ref[0], r) * block
            for part in range(2):
                rows = pl.ds(pl.multiple_of(part * size + source, block), block)
                for k in range(group):
                    if r == 0:
                        value = own_ref[part, me_ref[0] * count + first + k]
                    else:
                        value = pieces[r - 1][part, first + k]
                    if direct:
                        col_out[rows, lanes_of(base, k * times, times)] = value
                    else:
                        place[rows, pl.ds(k * times, times)] = value.astype(place.dtype)
        if not direct:
            col_out[:, lanes_of(base, 0, width)] = place[...].astype(col_out.dtype)
        sigma_into(sig, row_ref, col_out, base, 16, min(SPAN, width))
        acc[...] += overlap(sig[...], col_out[:, lanes_of(base, 0, width)])

    each_group(col_out.shape[1], width, body)
    if last:
        real = finish_sum(acc, before_ref, known_ref, rho_out, step_length)
        spread_rows(level_out, diagonal_row(real))


def later_kernel(last, row_ref, col_ref, low_ref, *refs):
    if last:
        before_ref, col_out, sum_out, acc, sig = refs
    else:
        col_out, acc, sig = refs
    low = low_ref[...]
    width = sig.shape[1]
    acc[...] = jnp.zeros_like(acc)

    def body(base):
        advance_into(col_out, low, col_ref, base, width)
        sigma_into(sig, row_ref, col_out, base, 16, min(SPAN, width))
        acc[...] += overlap(sig[...], col_out[:, lanes_of(base, 0, width)])

    each_group(col_out.shape[1], width, body)
    if last:
        finish_sum(acc, before_ref, None, sum_out, step_length)


def row_kernel(width, row_ref, low_ref, row_out):
    low = row_form(low_ref[...])
    each_group(row_ref.shape[1], width, lambda base: advance_into(row_out, low, row_ref, base, width))


def last_kernel(parts, me_ref, col_ref, low_ref, *refs):
    outs, moved = refs[:parts], refs[parts]
    _, _, block, times = outs[0].shape
    width = moved.shape[1]
    size = moved.shape[0] // 2
    low = low_ref[...]

    def body(base):
        first = lax.div(base, times)
        advance_into(moved, low, col_ref, base, width, local=True)
        for r in range(parts):
            target = lax.bitwise_xor(me_ref[0], r) * block
            for part in range(2):
                rows = pl.ds(pl.multiple_of(part * size + target, block), block)
                for k in range(width // times):
                    outs[r][part, first + k] = moved[rows, pl.ds(k * times, times)].astype(outs[r].dtype)

    each_group(col_ref.shape[1], width, body)


def cost(arrays, products):
    return pl.CostEstimate(flops=products * 2 * 256 * 256 * 4096, bytes_accessed=arrays * 2**21, transcendentals=0)


def place_type(block):
    return jnp.bfloat16 if block % 16 == 0 else jnp.float32


def sum_scratch(size, width):
    return [pltpu.VMEM((2 * size, 2 * size), jnp.float32), pltpu.VMEM((2 * size, width), jnp.bfloat16)]


def now_step(me, row, own, pieces, before=None, known=None, devices=0):
    size = own.shape[1]
    _, count, block, times = pieces[0].shape
    width = min(GROUP, count) * times
    square, history = ((2 * size, 2 * size), jnp.float32), (row.shape, jnp.bfloat16)
    args = (me, row, own, *pieces)
    place = pltpu.VMEM((2 * size, width), place_type(block))
    sig = pltpu.VMEM((2 * size, width), jnp.bfloat16)
    body = functools.partial(now_kernel, len(pieces) + 1, before is not None)
    if before is None:
        return call(body, [history, square], args, cost(4, 2), "now_step", [sig, place], 1)
    outs = [history, ((2, size, size), jnp.float32), ((devices, 1, size), jnp.float32)]
    scratch = sum_scratch(size, width) + [place]
    return call(body, outs, args + (before, known), cost(4, 2), "now_step", scratch, 1)


def later_step(row, col, low, width, before=None):
    double = row.shape[0]
    square, history = ((double, double), jnp.float32), (row.shape, jnp.bfloat16)
    sig = pltpu.VMEM((double, width), jnp.bfloat16)
    body = functools.partial(later_kernel, before is not None)
    if before is None:
        return call(body, [history, square], (row, col, low), cost(3, 2), "later_step", [sig])
    outs = [history, ((2, double // 2, double // 2), jnp.float32)]
    return call(body, outs, (row, col, low, before), cost(3, 2), "later_step", sum_scratch(double // 2, width))


def row_step(row, low, width):
    body = functools.partial(row_kernel, width)
    return call(body, [(row.shape, jnp.bfloat16)], (row, low), cost(2, 1), "row_step")[0]


def last_step(me, col, low, parts, count, times):
    double = col.shape[0]
    block = double // 2 // parts
    width = min(GROUP, count) * times
    outs = [((2, count, block, times), jnp.bfloat16)] * parts
    scratch = [pltpu.VMEM((double, width), place_type(block))]
    body = functools.partial(last_kernel, parts)
    return call(body, outs, (me, col, low), cost(2, 1), "last_step", scratch, 1)


def tree_sum(values):
    while len(values) > 1:
        values = [values[i] + values[i + 1] for i in range(0, len(values), 2)]
    return values[0]


def swap(value, name, r):
    return lax.ppermute(value, name, [(j, j ^ r) for j in range(lax.axis_size(name))])


def part_total(values):
    count = lax.axis_size("hist")
    rows = values.reshape(count, -1, values.shape[-1])
    share = jnp.sum(lax.all_to_all(rows, "hist", 0, 0, tiled=True), axis=0)
    return share


def whole_total(share, shape):
    count = lax.axis_size("hist")
    moved = [share] + [swap(share, "col", r) for r in range(1, lax.axis_size("col"))]
    share = tree_sum(moved)
    return lax.all_to_all(jnp.broadcast_to(share, (count,) + share.shape), "hist", 0, 0, tiled=True).reshape(shape)


def finish_rotation(left, unit):
    high = functools.partial(jnp.dot, precision=HIGH)
    real = high(left[0], unit[0].T) + high(left[1], unit[1].T)
    imag = high(left[1], unit[0].T) - high(left[0], unit[1].T)
    return jnp.stack([real, imag])


def rotate(unit, rho):
    high = functools.partial(jnp.dot, precision=HIGH)
    real = high(unit[0], rho[0]) - high(unit[1], rho[1])
    imag = high(unit[0], rho[1]) + high(unit[1], rho[0])
    return finish_rotation((real, imag), unit)


def gather_pieces(col):
    me, parts = lax.axis_index("col"), lax.axis_size("col")
    count = col.shape[1] // parts
    pieces = []
    for r in range(1, parts):
        piece = lax.dynamic_slice_in_dim(col, (me ^ r) * count, count, axis=1)
        pieces.append(swap(piece, "col", r))
    return pieces


def return_pieces(pieces):
    me, parts = lax.axis_index("col"), lax.axis_size("col")
    _, count, block, times = pieces[0].shape
    out = jnp.zeros((2, parts * count, block, times), pieces[0].dtype)
    for r, piece in enumerate(pieces):
        moved = piece if r == 0 else swap(piece, "col", r)
        out = lax.dynamic_update_slice_in_dim(out, moved, (me ^ r) * count, axis=1)
    return out


def per_device(less_row, less_col, great_row, great_col, density, hamiltonian):
    size, count, times = less_row.shape[1:]
    parts = lax.axis_size("col")
    devices = parts * lax.axis_size("hist")
    me = lax.axis_index("col").astype(jnp.int32).reshape(1)
    width = min(GROUP, count) * times

    great_pieces = gather_pieces(great_col)
    less_pieces = gather_pieces(less_col)

    symmetric = 0.5 * (hamiltonian + hamiltonian.T)
    low, unit = solve(diagonal_row(density[0]).reshape(1, 1, size), symmetric)
    known = rotate(unit, density * (1.0 / devices))

    less = less_row.reshape(2 * size, count * times)
    great = great_row.reshape(2 * size, count * times)
    less_next = row_step(less, low, width)
    great_next = row_step(great, low, width)
    cols_great, minus = now_step(me, less, great_col, great_pieces)
    cols_great, minus_later = later_step(less_next, cols_great, low, width)
    cols_less, rho, part = now_step(me, great, less_col, less_pieces, minus, known, devices)

    levels = lax.all_to_all(part, ("hist", "col"), 0, 0, tiled=True)
    cols_less, later = later_step(great_next, cols_less, low, width, minus_later)
    low, unit, left, part = solve(levels, symmetric, rho, later)

    levels = lax.all_to_all(part, ("hist", "col"), 0, 0, tiled=True)
    less_next = row_step(less_next, low, width)
    great_next = row_step(great_next, low, width)
    cols_great, minus = later_step(less_next, cols_great, low, width)
    cols_less, last = later_step(great_next, cols_less, low, width, minus)
    low, unit_last = solve(levels, symmetric)

    great_out = last_step(me, cols_great, low, parts, count, times)
    left, unit, later, last, unit_last, great_out = lax.optimization_barrier(
        (left, unit, later, last, unit_last, great_out)
    )
    rho = finish_rotation(left, unit) + later
    share = part_total(rotate(unit_last, rho) + last)
    cols_less, share = lax.optimization_barrier((cols_less, share))
    less_out = last_step(me, cols_less, low, parts, count, times)
    rho = whole_total(share, rho.shape)
    less_row_out = row_step(less_next, low, width).reshape(less_row.shape)
    great_row_out = row_step(great_next, low, width).reshape(great_row.shape)
    return (less_row_out, return_pieces(less_out), great_row_out, return_pieces(great_out), rho)


def solution(mesh):
    history = P(None, None, "col", "hist")
    return jax.shard_map(
        per_device,
        mesh=mesh,
        in_specs=(history, history, history, history, P(), P()),
        out_specs=(history, history, history, history, P()),
        check_vma=False,
    )
```

```python
import functools

import jax
import jax.numpy as jnp
from jax import lax
from jax.experimental import pallas as pl
from jax.experimental.pallas import tpu as pltpu
from jax.sharding import PartitionSpec as P


step_length = 0.1
mean_field = 2.0
coupling = 1.0

HIGH = lax.Precision.HIGHEST
SUBLANES = 8
GROUP = 8
SPAN = 256


def dot_high(a, b):
    return jnp.dot(a, b, precision=HIGH, preferred_element_type=jnp.float32)


def eye_mask(size):
    rows = lax.broadcasted_iota(jnp.int32, (size, size), 0)
    return rows == lax.broadcasted_iota(jnp.int32, (size, size), 1)


def inverse(matrix):
    size = matrix.shape[0]
    blocks = [matrix[p : p + SUBLANES] for p in range(0, size, SUBLANES)]
    rows = lax.broadcasted_iota(jnp.int32, (SUBLANES, size), 0)
    lanes = lax.broadcasted_iota(jnp.int32, (SUBLANES, size), 1)
    for p in range(len(blocks)):
        first = p * SUBLANES
        pivot_lanes = (lanes >= first) & (lanes < first + SUBLANES)

        def columns(block):
            return [jnp.broadcast_to(block[:, first + c : first + c + 1], (SUBLANES, size)) for c in range(SUBLANES)]

        pivot = columns(blocks[p])
        row_block = jnp.where(pivot_lanes, jnp.where(lanes == rows + first, 1.0, 0.0), blocks[p])
        for j in range(SUBLANES):

            def across(value):
                return jnp.broadcast_to(value[j : j + 1], (SUBLANES, size))

            scale = 1.0 / across(pivot[j])
            factor = pivot[j]

            def eliminate(value):
                top = across(value) * scale
                return jnp.where(rows == j, top, value - factor * top)

            row_block = eliminate(row_block)
            pivot = [eliminate(value) if c > j else value for c, value in enumerate(pivot)]
        spread = [jnp.broadcast_to(row_block[c : c + 1], (SUBLANES, size)) for c in range(SUBLANES)]
        order = list(range(p + 1, len(blocks))) + list(range(p))
        for q in order:
            total = jnp.where(pivot_lanes, 0.0, blocks[q])
            for c, column in enumerate(columns(blocks[q])):
                total = total - column * spread[c]
            blocks[q] = total
        blocks[p] = row_block
    return jnp.concatenate(blocks, axis=0)


def spread_rows(ref, row):
    ref[...] = jnp.broadcast_to(row.reshape(1, 1, row.shape[-1]), ref.shape)


def diagonal_row(matrix):
    return jnp.sum(jnp.where(eye_mask(matrix.shape[0]), matrix, 0.0), axis=0, keepdims=True)


def solve_kernel(rotates, levels_ref, ham_ref, *refs):
    size = ham_ref.shape[0]
    eye = eye_mask(size)
    level = levels_ref[0]
    for row in range(1, levels_ref.shape[0]):
        level = level + levels_ref[row]
    halved = (0.5 * step_length) * (ham_ref[...] + mean_field * jnp.where(eye, level, 0.0))
    identity = jnp.where(eye, 1.0, 0.0)
    solved = inverse(identity + dot_high(halved, halved))
    unit_real = 2.0 * solved - identity
    unit_imag = -2.0 * dot_high(solved, halved)
    low_real, low_imag = unit_real.astype(jnp.bfloat16), unit_imag.astype(jnp.bfloat16)
    if rotates:
        rho_ref, later_ref, low_ref, unit_ref, left_ref, next_ref = refs
    else:
        low_ref, unit_ref = refs
    low_ref[0:size, 0:size] = low_real
    low_ref[0:size, size:] = low_imag
    low_ref[size:, 0:size] = -low_imag
    low_ref[size:, size:] = low_real
    unit_ref[0] = unit_real
    unit_ref[1] = unit_imag
    if rotates:
        rho_real, rho_imag = rho_ref[0], rho_ref[1]
        left_real = dot_high(unit_real, rho_real) - dot_high(unit_imag, rho_imag)
        left_imag = dot_high(unit_real, rho_imag) + dot_high(unit_imag, rho_real)
        left_ref[0] = left_real
        left_ref[1] = left_imag
        real_diagonal = jnp.sum(left_real * unit_real + left_imag * unit_imag, axis=1, keepdims=True)
        row = jnp.sum(jnp.where(eye, real_diagonal + later_ref[0], 0.0), axis=0, keepdims=True)
        spread_rows(next_ref, row)


IN_VMEM = pl.BlockSpec(memory_space=pltpu.VMEM)
GRANT = pltpu.CompilerParams(vmem_limit_bytes=8 * 2**20)


def call(body, outs, args, cost_estimate, scratch=(), scalars=0):
    specs = [pl.BlockSpec(memory_space=pltpu.SMEM)] * scalars + [IN_VMEM] * (len(args) - scalars)
    return pl.pallas_call(
        body,
        out_shape=[jax.ShapeDtypeStruct(shape, kind) for shape, kind in outs],
        in_specs=specs,
        out_specs=[IN_VMEM] * len(outs),
        scratch_shapes=list(scratch),
        cost_estimate=cost_estimate,
        compiler_params=GRANT,
    )(*args)


def solve(levels, hamiltonian, rho=None, later=None):
    size = hamiltonian.shape[0]
    outs = [((2 * size, 2 * size), jnp.bfloat16), ((2, size, size), jnp.float32)]
    args = (levels, hamiltonian)
    if rho is not None:
        outs += [((2, size, size), jnp.float32), (levels.shape, jnp.float32)]
        args += (rho, later)
    estimate = pl.CostEstimate(flops=4_000_000_000, bytes_accessed=1_000_000, transcendentals=0)
    return call(functools.partial(solve_kernel, rho is not None), outs, args, estimate)


def lanes_of(base, first, span):
    return pl.ds(pl.multiple_of(base + first, 128), span)


def sigma_into(sig_ref, row_ref, col_ref, base, rows, span):
    size = sig_ref.shape[0] // 2
    for start in range(0, size, rows):
        for first in range(0, sig_ref.shape[1], span):
            real, imag = pl.ds(start, rows), pl.ds(size + start, rows)
            lanes, here = lanes_of(base, first, span), pl.ds(first, span)
            green_real = row_ref[real, lanes].astype(jnp.float32)
            green_imag = row_ref[imag, lanes].astype(jnp.float32)
            other_real = col_ref[real, lanes].astype(jnp.float32)
            other_imag = col_ref[imag, lanes].astype(jnp.float32)
            square_real = (coupling * coupling) * (green_real * green_real - green_imag * green_imag)
            square_imag = (coupling * coupling * 2.0) * green_real * green_imag
            sig_ref[real, here] = (square_real * other_real - square_imag * other_imag).astype(jnp.bfloat16)
            sig_ref[imag, here] = (square_real * other_imag + square_imag * other_real).astype(jnp.bfloat16)


def overlap(sig, col):
    return lax.dot_general(sig, col, (((1,), (1,)), ((), ())), preferred_element_type=jnp.float32)


def advance_into(out_ref, low, source_ref, base, width, local=False):
    span = min(SPAN, width)
    for first in range(0, width, span):
        lanes = lanes_of(base, first, span)
        target = pl.ds(first, span) if local else lanes
        moved = jnp.dot(low, source_ref[:, lanes], preferred_element_type=jnp.float32)
        out_ref[:, target] = moved.astype(out_ref.dtype)


def row_form(low):
    size = low.shape[0] // 2
    top = jnp.concatenate([low[:size, :size], low[size:, :size]], axis=1)
    bottom = jnp.concatenate([low[:size, size:], low[:size, :size]], axis=1)
    return jnp.concatenate([top, bottom], axis=0)


def each_group(total_width, width, body):
    def step(g, carry):
        body(pl.multiple_of(g * width, width))
        return carry

    lax.fori_loop(0, total_width // width, step, 0)


def complex_sum(four):
    size = four.shape[0] // 2
    return four[:size, :size] - four[size:, size:], four[:size, size:] + four[size:, :size]


def finish_sum(acc, before_ref, base_ref, out_ref, scale):
    real, imag = complex_sum(scale * (acc[...] - before_ref[...]))
    if base_ref is not None:
        real, imag = base_ref[0] + real, base_ref[1] + imag
    out_ref[0] = real
    out_ref[1] = imag
    return real


def now_kernel(parts, last, me_ref, row_ref, own_ref, *refs):
    pieces, refs = refs[: parts - 1], refs[parts - 1 :]
    if last:
        before_ref, known_ref, col_out, rho_out, level_out, acc, sig, place = refs
    else:
        col_out, acc, sig, place = refs
    _, count, block, times = pieces[0].shape
    width = sig.shape[1]
    group = width // times
    size = sig.shape[0] // 2
    direct = place.dtype == col_out.dtype
    acc[...] = jnp.zeros_like(acc)

    def body(base):
        first = lax.div(base, times)
        for r in range(parts):
            source = lax.bitwise_xor(me_ref[0], r) * block
            for part in range(2):
                rows = pl.ds(pl.multiple_of(part * size + source, block), block)
                for k in range(group):
                    if r == 0:
                        value = own_ref[part, me_ref[0] * count + first + k]
                    else:
                        value = pieces[r - 1][part, first + k]
                    if direct:
                        col_out[rows, lanes_of(base, k * times, times)] = value
                    else:
                        place[rows, pl.ds(k * times, times)] = value.astype(place.dtype)
        if not direct:
            col_out[:, lanes_of(base, 0, width)] = place[...].astype(col_out.dtype)
        sigma_into(sig, row_ref, col_out, base, 16, min(SPAN, width))
        acc[...] += overlap(sig[...], col_out[:, lanes_of(base, 0, width)])

    each_group(col_out.shape[1], width, body)
    if last:
        real = finish_sum(acc, before_ref, known_ref, rho_out, step_length)
        spread_rows(level_out, diagonal_row(real))


def later_kernel(last, row_ref, col_ref, low_ref, *refs):
    if last:
        before_ref, row_out, col_out, sum_out, acc, sig = refs
    else:
        row_out, col_out, acc, sig = refs
    width = sig.shape[1]
    acc[...] = jnp.zeros_like(acc)

    def body(base):
        advance_into(row_out, row_form(low_ref[...]), row_ref, base, width)
        advance_into(col_out, low_ref[...], col_ref, base, width)
        sigma_into(sig, row_out, col_out, base, 16, min(SPAN, width))
        acc[...] += overlap(sig[...], col_out[:, lanes_of(base, 0, width)])

    each_group(col_out.shape[1], width, body)
    if last:
        finish_sum(acc, before_ref, None, sum_out, step_length)


def finish_kernel(left_ref, unit_ref, later_ref, unit_last_ref, last_ref, rho_ref):
    def right(real, imag, unit):
        turned_real, turned_imag = unit[0].T, unit[1].T
        return (
            dot_high(real, turned_real) + dot_high(imag, turned_imag),
            dot_high(imag, turned_real) - dot_high(real, turned_imag),
        )

    real, imag = right(left_ref[0], left_ref[1], unit_ref)
    real, imag = real + later_ref[0], imag + later_ref[1]
    unit_real, unit_imag = unit_last_ref[0], unit_last_ref[1]
    left_real = dot_high(unit_real, real) - dot_high(unit_imag, imag)
    left_imag = dot_high(unit_real, imag) + dot_high(unit_imag, real)
    real, imag = right(left_real, left_imag, unit_last_ref)
    rho_ref[0] = real + last_ref[0]
    rho_ref[1] = imag + last_ref[1]


def row_kernel(width, row_ref, low_ref, row_out):
    low = row_form(low_ref[...])
    each_group(row_ref.shape[1], width, lambda base: advance_into(row_out, low, row_ref, base, width))


def last_kernel(parts, me_ref, col_ref, low_ref, *refs):
    outs, moved = refs[:parts], refs[parts]
    _, _, block, times = outs[0].shape
    width = moved.shape[1]
    size = moved.shape[0] // 2
    low = low_ref[...]

    def body(base):
        first = lax.div(base, times)
        advance_into(moved, low, col_ref, base, width, local=True)
        for r in range(parts):
            target = lax.bitwise_xor(me_ref[0], r) * block
            for part in range(2):
                rows = pl.ds(pl.multiple_of(part * size + target, block), block)
                for k in range(width // times):
                    outs[r][part, first + k] = moved[rows, pl.ds(k * times, times)].astype(outs[r].dtype)

    each_group(col_ref.shape[1], width, body)


def cost(arrays, products):
    return pl.CostEstimate(flops=products * 2 * 256 * 256 * 4096, bytes_accessed=arrays * 2**21, transcendentals=0)


def place_type(block):
    return jnp.bfloat16 if block % 16 == 0 else jnp.float32


def sum_scratch(size, width):
    return [pltpu.VMEM((2 * size, 2 * size), jnp.float32), pltpu.VMEM((2 * size, width), jnp.bfloat16)]


def now_step(me, row, own, pieces, before=None, known=None, devices=0):
    size = own.shape[1]
    _, count, block, times = pieces[0].shape
    width = min(GROUP, count) * times
    square, history = ((2 * size, 2 * size), jnp.float32), (row.shape, jnp.bfloat16)
    args = (me, row, own, *pieces)
    place = pltpu.VMEM((2 * size, width), place_type(block))
    sig = pltpu.VMEM((2 * size, width), jnp.bfloat16)
    body = functools.partial(now_kernel, len(pieces) + 1, before is not None)
    if before is None:
        return call(body, [history, square], args, cost(4, 2), [sig, place], 1)
    outs = [history, ((2, size, size), jnp.float32), ((devices, 1, size), jnp.float32)]
    scratch = sum_scratch(size, width) + [place]
    return call(body, outs, args + (before, known), cost(4, 2), scratch, 1)


def later_step(row, col, low, width, before=None):
    double = row.shape[0]
    square, history = ((double, double), jnp.float32), (row.shape, jnp.bfloat16)
    body = functools.partial(later_kernel, before is not None)
    if before is None:
        scratch = [pltpu.VMEM((double, width), jnp.bfloat16)]
        return call(body, [history, history, square], (row, col, low), cost(4, 3), scratch)
    outs = [history, history, ((2, double // 2, double // 2), jnp.float32)]
    return call(body, outs, (row, col, low, before), cost(4, 3), sum_scratch(double // 2, width))


def row_step(row, low, width):
    body = functools.partial(row_kernel, width)
    return call(body, [(row.shape, jnp.bfloat16)], (row, low), cost(2, 1))[0]


def last_step(me, col, low, parts, count, times):
    double = col.shape[0]
    block = double // 2 // parts
    width = min(GROUP, count) * times
    outs = [((2, count, block, times), jnp.bfloat16)] * parts
    scratch = [pltpu.VMEM((double, width), place_type(block))]
    body = functools.partial(last_kernel, parts)
    return call(body, outs, (me, col, low), cost(2, 1), scratch, 1)


def tree_sum(values):
    while len(values) > 1:
        values = [values[i] + values[i + 1] for i in range(0, len(values), 2)]
    return values[0]


def swap(value, name, r):
    return lax.ppermute(value, name, [(j, j ^ r) for j in range(lax.axis_size(name))])


def part_total(values):
    count = lax.axis_size("hist")
    rows = values.reshape(count, -1, values.shape[-1])
    share = jnp.sum(lax.all_to_all(rows, "hist", 0, 0, tiled=True), axis=0)
    return share


def whole_total(share, shape):
    count = lax.axis_size("hist")
    moved = [share] + [swap(share, "col", r) for r in range(1, lax.axis_size("col"))]
    share = tree_sum(moved)
    return lax.all_to_all(jnp.broadcast_to(share, (count,) + share.shape), "hist", 0, 0, tiled=True).reshape(shape)


def finish_rotation(left, unit):
    high = functools.partial(jnp.dot, precision=HIGH)
    real = high(left[0], unit[0].T) + high(left[1], unit[1].T)
    imag = high(left[1], unit[0].T) - high(left[0], unit[1].T)
    return jnp.stack([real, imag])


def rotate(unit, rho):
    high = functools.partial(jnp.dot, precision=HIGH)
    real = high(unit[0], rho[0]) - high(unit[1], rho[1])
    imag = high(unit[0], rho[1]) + high(unit[1], rho[0])
    return finish_rotation((real, imag), unit)


def gather_pieces(col):
    me, parts = lax.axis_index("col"), lax.axis_size("col")
    count = col.shape[1] // parts
    pieces = []
    for r in range(1, parts):
        piece = lax.dynamic_slice_in_dim(col, (me ^ r) * count, count, axis=1)
        pieces.append(swap(piece, "col", r))
    return pieces


def return_pieces(pieces):
    me, parts = lax.axis_index("col"), lax.axis_size("col")
    _, count, block, times = pieces[0].shape
    out = jnp.zeros((2, parts * count, block, times), pieces[0].dtype)
    for r, piece in enumerate(pieces):
        moved = piece if r == 0 else swap(piece, "col", r)
        out = lax.dynamic_update_slice_in_dim(out, moved, (me ^ r) * count, axis=1)
    return out


def per_device(less_row, less_col, great_row, great_col, density, hamiltonian):
    size, count, times = less_row.shape[1:]
    parts = lax.axis_size("col")
    devices = parts * lax.axis_size("hist")
    me = lax.axis_index("col").astype(jnp.int32).reshape(1)
    width = min(GROUP, count) * times

    great_pieces = gather_pieces(great_col)
    less_pieces = gather_pieces(less_col)

    symmetric = 0.5 * (hamiltonian + hamiltonian.T)
    low, unit = solve(diagonal_row(density[0]).reshape(1, 1, size), symmetric)
    known = rotate(unit, density * (1.0 / devices))

    less = less_row.reshape(2 * size, count * times)
    great = great_row.reshape(2 * size, count * times)
    cols_great, minus = now_step(me, less, great_col, great_pieces)
    less, cols_great, minus_later = later_step(less, cols_great, low, width)
    less_pieces, minus_later = lax.optimization_barrier((less_pieces, minus_later))
    cols_less, rho, part = now_step(me, great, less_col, less_pieces, minus, known, devices)

    levels = lax.all_to_all(part, ("hist", "col"), 0, 0, tiled=True)
    great, cols_less, later = later_step(great, cols_less, low, width, minus_later)
    low, unit, left, part = solve(levels, symmetric, rho, later)

    levels = lax.all_to_all(part, ("hist", "col"), 0, 0, tiled=True)
    less, cols_great, minus = later_step(less, cols_great, low, width)
    great, cols_less, last = later_step(great, cols_less, low, width, minus)
    low, unit_last = solve(levels, symmetric)

    great_out = return_pieces(last_step(me, cols_great, low, parts, count, times))
    args = (left, unit, later, unit_last, last)
    estimate = pl.CostEstimate(flops=500_000_000, bytes_accessed=1_000_000, transcendentals=0)
    rho = call(finish_kernel, [(density.shape, jnp.float32)], args, estimate)[0]
    share = part_total(rho)
    cols_less, share = lax.optimization_barrier((cols_less, share))
    less_out = return_pieces(last_step(me, cols_less, low, parts, count, times))
    rho = whole_total(share, density.shape)
    less_row_out = row_step(less, low, width).reshape(less_row.shape)
    great_row_out = row_step(great, low, width).reshape(great_row.shape)
    return (less_row_out, less_out, great_row_out, great_out, rho)


def solution(mesh):
    history = P(None, None, "col", "hist")
    return jax.shard_map(
        per_device,
        mesh=mesh,
        in_specs=(history, history, history, history, P(), P()),
        out_specs=(history, history, history, history, P()),
        check_vma=False,
    )
```

```python
import functools

import jax
import jax.numpy as jnp
from jax import lax
from jax.experimental import pallas as pl
from jax.experimental.pallas import tpu as pltpu
from jax.sharding import PartitionSpec as P


step_length = 0.1
mean_field = 2.0
coupling = 1.0

HIGH = lax.Precision.HIGHEST
SUBLANES = 8
GROUP = 8
SPAN = 256


def dot_high(a, b):
    return jnp.dot(a, b, precision=HIGH, preferred_element_type=jnp.float32)


def eye_mask(size):
    rows = lax.broadcasted_iota(jnp.int32, (size, size), 0)
    return rows == lax.broadcasted_iota(jnp.int32, (size, size), 1)


def inverse(matrix):
    size = matrix.shape[0]
    blocks = [matrix[p : p + SUBLANES] for p in range(0, size, SUBLANES)]
    rows = lax.broadcasted_iota(jnp.int32, (SUBLANES, size), 0)
    lanes = lax.broadcasted_iota(jnp.int32, (SUBLANES, size), 1)
    for p in range(len(blocks)):
        first = p * SUBLANES
        pivot_lanes = (lanes >= first) & (lanes < first + SUBLANES)

        def columns(block):
            return [jnp.broadcast_to(block[:, first + c : first + c + 1], (SUBLANES, size)) for c in range(SUBLANES)]

        pivot = columns(blocks[p])
        row_block = jnp.where(pivot_lanes, jnp.where(lanes == rows + first, 1.0, 0.0), blocks[p])
        for j in range(SUBLANES):

            def across(value):
                return jnp.broadcast_to(value[j : j + 1], (SUBLANES, size))

            scale = 1.0 / across(pivot[j])
            factor = pivot[j]

            def eliminate(value):
                top = across(value) * scale
                return jnp.where(rows == j, top, value - factor * top)

            row_block = eliminate(row_block)
            pivot = [eliminate(value) if c > j else value for c, value in enumerate(pivot)]
        spread = [jnp.broadcast_to(row_block[c : c + 1], (SUBLANES, size)) for c in range(SUBLANES)]
        order = list(range(p + 1, len(blocks))) + list(range(p))
        for q in order:
            total = jnp.where(pivot_lanes, 0.0, blocks[q])
            for c, column in enumerate(columns(blocks[q])):
                total = total - column * spread[c]
            blocks[q] = total
        blocks[p] = row_block
    return jnp.concatenate(blocks, axis=0)


def spread_rows(ref, row):
    ref[...] = jnp.broadcast_to(row.reshape(1, 1, row.shape[-1]), ref.shape)


def diagonal_row(matrix):
    return jnp.sum(jnp.where(eye_mask(matrix.shape[0]), matrix, 0.0), axis=0, keepdims=True)


def solve_kernel(rotates, levels_ref, ham_ref, *refs):
    size = ham_ref.shape[0]
    eye = eye_mask(size)
    level = levels_ref[0]
    for row in range(1, levels_ref.shape[0]):
        level = level + levels_ref[row]
    halved = (0.5 * step_length) * (ham_ref[...] + mean_field * jnp.where(eye, level, 0.0))
    identity = jnp.where(eye, 1.0, 0.0)
    solved = inverse(identity + dot_high(halved, halved))
    unit_real = 2.0 * solved - identity
    unit_imag = -2.0 * dot_high(solved, halved)
    low_real, low_imag = unit_real.astype(jnp.bfloat16), unit_imag.astype(jnp.bfloat16)
    if rotates:
        rho_ref, later_ref, low_ref, unit_ref, left_ref, next_ref = refs
    else:
        low_ref, unit_ref = refs
    low_ref[0:size, 0:size] = low_real
    low_ref[0:size, size:] = low_imag
    low_ref[size:, 0:size] = -low_imag
    low_ref[size:, size:] = low_real
    unit_ref[0] = unit_real
    unit_ref[1] = unit_imag
    if rotates:
        rho_real, rho_imag = rho_ref[0], rho_ref[1]
        left_real = dot_high(unit_real, rho_real) - dot_high(unit_imag, rho_imag)
        left_imag = dot_high(unit_real, rho_imag) + dot_high(unit_imag, rho_real)
        left_ref[0] = left_real
        left_ref[1] = left_imag
        real_diagonal = jnp.sum(left_real * unit_real + left_imag * unit_imag, axis=1, keepdims=True)
        row = jnp.sum(jnp.where(eye, real_diagonal + later_ref[0], 0.0), axis=0, keepdims=True)
        spread_rows(next_ref, row)


IN_VMEM = pl.BlockSpec(memory_space=pltpu.VMEM)
IN_HBM = pl.BlockSpec(memory_space=pl.ANY)


def call(body, outs, args, cost_estimate, scratch=(), scalars=0, streamed=(), streamed_outs=(), grant=8):
    specs = [pl.BlockSpec(memory_space=pltpu.SMEM)] * scalars
    specs += [IN_HBM if i in streamed else IN_VMEM for i in range(scalars, len(args))]
    return pl.pallas_call(
        body,
        out_shape=[
            pltpu.HBM(shape, kind) if i in streamed_outs else jax.ShapeDtypeStruct(shape, kind)
            for i, (shape, kind) in enumerate(outs)
        ],
        in_specs=specs,
        out_specs=[IN_HBM if i in streamed_outs else IN_VMEM for i in range(len(outs))],
        scratch_shapes=list(scratch),
        cost_estimate=cost_estimate,
        compiler_params=pltpu.CompilerParams(vmem_limit_bytes=grant * 2**20 if grant else None),
    )(*args)


def stream(outside, inside, semaphores, base, group, width, inward):
    lanes = lanes_of(base, 0, width)
    ends = (outside.at[:, lanes], inside.at[:, lanes])
    source, target = ends if inward else ends[::-1]
    return pltpu.make_async_copy(source, target, semaphores.at[group])


def solve(levels, hamiltonian, rho=None, later=None):
    size = hamiltonian.shape[0]
    outs = [((2 * size, 2 * size), jnp.bfloat16), ((2, size, size), jnp.float32)]
    args = (levels, hamiltonian)
    if rho is not None:
        outs += [((2, size, size), jnp.float32), (levels.shape, jnp.float32)]
        args += (rho, later)
    estimate = pl.CostEstimate(flops=4_000_000_000, bytes_accessed=1_000_000, transcendentals=0)
    return call(functools.partial(solve_kernel, rho is not None), outs, args, estimate)


def lanes_of(base, first, span):
    return pl.ds(pl.multiple_of(base + first, 128), span)


def sigma_into(sig_ref, row_ref, col_ref, base, rows, span):
    size = sig_ref.shape[0] // 2
    for start in range(0, size, rows):
        for first in range(0, sig_ref.shape[1], span):
            real, imag = pl.ds(start, rows), pl.ds(size + start, rows)
            lanes, here = lanes_of(base, first, span), pl.ds(first, span)
            green_real = row_ref[real, lanes].astype(jnp.float32)
            green_imag = row_ref[imag, lanes].astype(jnp.float32)
            other_real = col_ref[real, lanes].astype(jnp.float32)
            other_imag = col_ref[imag, lanes].astype(jnp.float32)
            square_real = (coupling * coupling) * (green_real * green_real - green_imag * green_imag)
            square_imag = (coupling * coupling * 2.0) * green_real * green_imag
            sig_ref[real, here] = (square_real * other_real - square_imag * other_imag).astype(jnp.bfloat16)
            sig_ref[imag, here] = (square_real * other_imag + square_imag * other_real).astype(jnp.bfloat16)


def overlap(sig, col):
    return lax.dot_general(sig, col, (((1,), (1,)), ((), ())), preferred_element_type=jnp.float32)


def advance_into(out_ref, low, source_ref, base, width, local=False):
    span = min(SPAN, width)
    for first in range(0, width, span):
        lanes = lanes_of(base, first, span)
        target = pl.ds(first, span) if local else lanes
        moved = jnp.dot(low, source_ref[:, lanes], preferred_element_type=jnp.float32)
        out_ref[:, target] = moved.astype(out_ref.dtype)


def row_form(low):
    size = low.shape[0] // 2
    top = jnp.concatenate([low[:size, :size], low[size:, :size]], axis=1)
    bottom = jnp.concatenate([low[:size, size:], low[:size, :size]], axis=1)
    return jnp.concatenate([top, bottom], axis=0)


def each_group(total_width, width, body):
    def step(g, carry):
        body(pl.multiple_of(g * width, width), g)
        return carry

    lax.fori_loop(0, total_width // width, step, 0)


def complex_sum(four):
    size = four.shape[0] // 2
    return four[:size, :size] - four[size:, size:], four[:size, size:] + four[size:, :size]


def finish_sum(acc, before_ref, base_ref, out_ref, scale):
    real, imag = complex_sum(scale * (acc[...] - before_ref[...]))
    if base_ref is not None:
        real, imag = base_ref[0] + real, base_ref[1] + imag
    out_ref[0] = real
    out_ref[1] = imag
    return real


def now_kernel(parts, last, me_ref, row_ref, own_ref, *refs):
    pieces, refs = refs[: parts - 1], refs[parts - 1 :]
    if last:
        before_ref, known_ref, col_hbm, rho_out, level_out, acc, sig, place, col_out, sent = refs
    else:
        col_hbm, acc, sig, place, col_out, sent = refs
    _, count, block, times = pieces[0].shape
    width = sig.shape[1]
    group = width // times
    size = sig.shape[0] // 2
    direct = place.dtype == col_out.dtype
    acc[...] = jnp.zeros_like(acc)

    def body(base, g):
        first = lax.div(base, times)
        for r in range(parts):
            source = lax.bitwise_xor(me_ref[0], r) * block
            for part in range(2):
                rows = pl.ds(pl.multiple_of(part * size + source, block), block)
                for k in range(group):
                    if r == 0:
                        value = own_ref[part, me_ref[0] * count + first + k]
                    else:
                        value = pieces[r - 1][part, first + k]
                    if direct:
                        col_out[rows, lanes_of(base, k * times, times)] = value
                    else:
                        place[rows, pl.ds(k * times, times)] = value.astype(place.dtype)
        if not direct:
            col_out[:, lanes_of(base, 0, width)] = place[...].astype(col_out.dtype)
        stream(col_hbm, col_out, sent, base, g, width, False).start()
        sigma_into(sig, row_ref, col_out, base, 16, min(SPAN, width))
        acc[...] += overlap(sig[...], col_out[:, lanes_of(base, 0, width)])

    each_group(col_out.shape[1], width, body)
    each_group(col_out.shape[1], width, lambda base, g: stream(col_hbm, col_out, sent, base, g, width, False).wait())
    if last:
        real = finish_sum(acc, before_ref, known_ref, rho_out, step_length)
        spread_rows(level_out, diagonal_row(real))


def later_kernel(last, row_hbm, col_hbm, low_ref, *refs):
    if last:
        before_ref, row_to, col_to, sum_out, acc, *refs = refs
    else:
        row_to, col_to, acc, *refs = refs
    sig, row_ref, col_ref, row_out, col_out, row_came, col_came, row_went, col_went = refs
    total_width, width = row_ref.shape[1], sig.shape[1]

    def loads(base, g):
        return (
            stream(row_hbm, row_ref, row_came, base, g, width, True),
            stream(col_hbm, col_ref, col_came, base, g, width, True),
        )

    def stores(base, g):
        return (
            stream(row_to, row_out, row_went, base, g, width, False),
            stream(col_to, col_out, col_went, base, g, width, False),
        )

    def start(base, g):
        for copy in loads(base, g):
            copy.start()

    def wait(base, g):
        for copy in stores(base, g):
            copy.wait()

    each_group(total_width, width, start)
    acc[...] = jnp.zeros_like(acc)

    def body(base, g):
        for copy in loads(base, g):
            copy.wait()
        advance_into(row_out, row_form(low_ref[...]), row_ref, base, width)
        advance_into(col_out, low_ref[...], col_ref, base, width)
        for copy in stores(base, g):
            copy.start()
        sigma_into(sig, row_out, col_out, base, 16, min(SPAN, width))
        acc[...] += overlap(sig[...], col_out[:, lanes_of(base, 0, width)])

    each_group(total_width, width, body)
    if last:
        finish_sum(acc, before_ref, None, sum_out, step_length)
    each_group(total_width, width, wait)


def finish_kernel(left_ref, unit_ref, later_ref, unit_last_ref, last_ref, rho_ref):
    def right(real, imag, unit):
        turned_real, turned_imag = unit[0].T, unit[1].T
        return (
            dot_high(real, turned_real) + dot_high(imag, turned_imag),
            dot_high(imag, turned_real) - dot_high(real, turned_imag),
        )

    real, imag = right(left_ref[0], left_ref[1], unit_ref)
    real, imag = real + later_ref[0], imag + later_ref[1]
    unit_real, unit_imag = unit_last_ref[0], unit_last_ref[1]
    left_real = dot_high(unit_real, real) - dot_high(unit_imag, imag)
    left_imag = dot_high(unit_real, imag) + dot_high(unit_imag, real)
    real, imag = right(left_real, left_imag, unit_last_ref)
    rho_ref[0] = real + last_ref[0]
    rho_ref[1] = imag + last_ref[1]


def row_kernel(width, row_ref, low_ref, row_out):
    low = row_form(low_ref[...])
    each_group(row_ref.shape[1], width, lambda base, g: advance_into(row_out, low, row_ref, base, width))


def last_kernel(parts, me_ref, col_ref, low_ref, *refs):
    outs, moved = refs[:parts], refs[parts]
    _, _, block, times = outs[0].shape
    width = moved.shape[1]
    size = moved.shape[0] // 2
    low = low_ref[...]

    def body(base, g):
        first = lax.div(base, times)
        advance_into(moved, low, col_ref, base, width, local=True)
        for r in range(parts):
            target = lax.bitwise_xor(me_ref[0], r) * block
            for part in range(2):
                rows = pl.ds(pl.multiple_of(part * size + target, block), block)
                for k in range(width // times):
                    outs[r][part, first + k] = moved[rows, pl.ds(k * times, times)].astype(outs[r].dtype)

    each_group(col_ref.shape[1], width, body)


def cost(arrays, products):
    return pl.CostEstimate(flops=products * 2 * 256 * 256 * 4096, bytes_accessed=arrays * 2**21, transcendentals=0)


def place_type(block):
    return jnp.bfloat16 if block % 16 == 0 else jnp.float32


def sum_scratch(size, width):
    return [pltpu.VMEM((2 * size, 2 * size), jnp.float32), pltpu.VMEM((2 * size, width), jnp.bfloat16)]


def now_step(me, row, own, pieces, before=None, known=None, devices=0):
    size = own.shape[1]
    _, count, block, times = pieces[0].shape
    width = min(GROUP, count) * times
    square, history = ((2 * size, 2 * size), jnp.float32), (row.shape, jnp.bfloat16)
    args = (me, row, own, *pieces)
    scratch = sum_scratch(size, width)
    scratch += [pltpu.VMEM((2 * size, width), place_type(block)), pltpu.VMEM(row.shape, jnp.bfloat16)]
    scratch += [pltpu.SemaphoreType.DMA((row.shape[1] // width,))]
    body = functools.partial(now_kernel, len(pieces) + 1, before is not None)
    if before is None:
        outs, scratch = [history, square], scratch[1:]
    else:
        outs, args = [history, ((2, size, size), jnp.float32), ((devices, 1, size), jnp.float32)], args + (before, known)
    return call(body, outs, args, cost(4, 2), scratch, 1, streamed_outs=(0,))


def later_step(row, col, low, width, before=None):
    double = row.shape[0]
    square, history = ((double, double), jnp.float32), (row.shape, jnp.bfloat16)
    body = functools.partial(later_kernel, before is not None)
    scratch = sum_scratch(double // 2, width) + [pltpu.VMEM(row.shape, jnp.bfloat16)] * 4
    scratch += [pltpu.SemaphoreType.DMA((row.shape[1] // width,))] * 4
    if before is None:
        outs, args, scratch = [history, history, square], (row, col, low), scratch[1:]
    else:
        outs, args = [history, history, ((2, double // 2, double // 2), jnp.float32)], (row, col, low, before)
    return call(body, outs, args, cost(4, 3), scratch, 0, (0, 1), (0, 1), None)


def row_step(row, low, width):
    body = functools.partial(row_kernel, width)
    return call(body, [(row.shape, jnp.bfloat16)], (row, low), cost(2, 1))[0]


def last_step(me, col, low, parts, count, times):
    double = col.shape[0]
    block = double // 2 // parts
    width = min(GROUP, count) * times
    outs = [((2, count, block, times), jnp.bfloat16)] * parts
    scratch = [pltpu.VMEM((double, width), place_type(block))]
    body = functools.partial(last_kernel, parts)
    return call(body, outs, (me, col, low), cost(2, 1), scratch, 1)


def tree_sum(values):
    while len(values) > 1:
        values = [values[i] + values[i + 1] for i in range(0, len(values), 2)]
    return values[0]


def swap(value, name, r):
    return lax.ppermute(value, name, [(j, j ^ r) for j in range(lax.axis_size(name))])


def part_total(values):
    count = lax.axis_size("hist")
    rows = values.reshape(count, -1, values.shape[-1])
    share = jnp.sum(lax.all_to_all(rows, "hist", 0, 0, tiled=True), axis=0)
    return share


def whole_total(share, shape):
    count = lax.axis_size("hist")
    moved = [share] + [swap(share, "col", r) for r in range(1, lax.axis_size("col"))]
    share = tree_sum(moved)
    return lax.all_to_all(jnp.broadcast_to(share, (count,) + share.shape), "hist", 0, 0, tiled=True).reshape(shape)


def finish_rotation(left, unit):
    high = functools.partial(jnp.dot, precision=HIGH)
    real = high(left[0], unit[0].T) + high(left[1], unit[1].T)
    imag = high(left[1], unit[0].T) - high(left[0], unit[1].T)
    return jnp.stack([real, imag])


def rotate(unit, rho):
    high = functools.partial(jnp.dot, precision=HIGH)
    real = high(unit[0], rho[0]) - high(unit[1], rho[1])
    imag = high(unit[0], rho[1]) + high(unit[1], rho[0])
    return finish_rotation((real, imag), unit)


def gather_pieces(col):
    me, parts = lax.axis_index("col"), lax.axis_size("col")
    count = col.shape[1] // parts
    pieces = []
    for r in range(1, parts):
        piece = lax.dynamic_slice_in_dim(col, (me ^ r) * count, count, axis=1)
        pieces.append(swap(piece, "col", r))
    return pieces


def return_pieces(pieces):
    me, parts = lax.axis_index("col"), lax.axis_size("col")
    _, count, block, times = pieces[0].shape
    out = jnp.zeros((2, parts * count, block, times), pieces[0].dtype)
    for r, piece in enumerate(pieces):
        moved = piece if r == 0 else swap(piece, "col", r)
        out = lax.dynamic_update_slice_in_dim(out, moved, (me ^ r) * count, axis=1)
    return out


def per_device(less_row, less_col, great_row, great_col, density, hamiltonian):
    size, count, times = less_row.shape[1:]
    parts = lax.axis_size("col")
    devices = parts * lax.axis_size("hist")
    me = lax.axis_index("col").astype(jnp.int32).reshape(1)
    width = min(GROUP, count) * times

    great_pieces = gather_pieces(great_col)
    less_pieces = gather_pieces(less_col)

    symmetric = 0.5 * (hamiltonian + hamiltonian.T)
    low, unit = solve(diagonal_row(density[0]).reshape(1, 1, size), symmetric)
    known = rotate(unit, density * (1.0 / devices))

    less = less_row.reshape(2 * size, count * times)
    great = great_row.reshape(2 * size, count * times)
    cols_great, minus = now_step(me, less, great_col, great_pieces)
    less, cols_great, minus_later = later_step(less, cols_great, low, width)
    less_pieces, minus_later = lax.optimization_barrier((less_pieces, minus_later))
    cols_less, rho, part = now_step(me, great, less_col, less_pieces, minus, known, devices)

    levels = lax.all_to_all(part, ("hist", "col"), 0, 0, tiled=True)
    great, cols_less, later = later_step(great, cols_less, low, width, minus_later)
    low, unit, left, part = solve(levels, symmetric, rho, later)

    levels = lax.all_to_all(part, ("hist", "col"), 0, 0, tiled=True)
    less, cols_great, minus = later_step(less, cols_great, low, width)
    low_last, unit_last = solve(levels, symmetric)

    great_out = return_pieces(last_step(me, cols_great, low_last, parts, count, times))
    great, cols_less, last = later_step(great, cols_less, low, width, minus)
    low = low_last
    args = (left, unit, later, unit_last, last)
    estimate = pl.CostEstimate(flops=500_000_000, bytes_accessed=1_000_000, transcendentals=0)
    rho = call(finish_kernel, [(density.shape, jnp.float32)], args, estimate)[0]
    share = part_total(rho)
    cols_less, share = lax.optimization_barrier((cols_less, share))
    less_out = return_pieces(last_step(me, cols_less, low, parts, count, times))
    rho = whole_total(share, density.shape)
    less_row_out = row_step(less, low, width).reshape(less_row.shape)
    great_row_out = row_step(great, low, width).reshape(great_row.shape)
    return (less_row_out, less_out, great_row_out, great_out, rho)


def solution(mesh):
    history = P(None, None, "col", "hist")
    return jax.shard_map(
        per_device,
        mesh=mesh,
        in_specs=(history, history, history, history, P(), P()),
        out_specs=(history, history, history, history, P()),
        check_vma=False,
    )
```

```python
import functools

import jax
import jax.numpy as jnp
from jax import lax
from jax.experimental import pallas as pl
from jax.experimental.pallas import tpu as pltpu
from jax.sharding import PartitionSpec as P


step_length = 0.1
mean_field = 2.0
coupling = 1.0

HIGH = lax.Precision.HIGHEST
SUBLANES = 8
GROUP = 8
SPAN = 256


def dot_high(a, b):
    return jnp.dot(a, b, precision=HIGH, preferred_element_type=jnp.float32)


def eye_mask(size):
    rows = lax.broadcasted_iota(jnp.int32, (size, size), 0)
    return rows == lax.broadcasted_iota(jnp.int32, (size, size), 1)


def inverse(matrix):
    size = matrix.shape[0]
    blocks = [matrix[p : p + SUBLANES] for p in range(0, size, SUBLANES)]
    rows = lax.broadcasted_iota(jnp.int32, (SUBLANES, size), 0)
    lanes = lax.broadcasted_iota(jnp.int32, (SUBLANES, size), 1)
    for p in range(len(blocks)):
        first = p * SUBLANES
        pivot_lanes = (lanes >= first) & (lanes < first + SUBLANES)

        def columns(block):
            return [jnp.broadcast_to(block[:, first + c : first + c + 1], (SUBLANES, size)) for c in range(SUBLANES)]

        pivot = columns(blocks[p])
        row_block = jnp.where(pivot_lanes, jnp.where(lanes == rows + first, 1.0, 0.0), blocks[p])
        for j in range(SUBLANES):

            def across(value):
                return jnp.broadcast_to(value[j : j + 1], (SUBLANES, size))

            scale = 1.0 / across(pivot[j])
            factor = pivot[j]

            def eliminate(value):
                top = across(value) * scale
                return jnp.where(rows == j, top, value - factor * top)

            row_block = eliminate(row_block)
            pivot = [eliminate(value) if c > j else value for c, value in enumerate(pivot)]
        spread = [jnp.broadcast_to(row_block[c : c + 1], (SUBLANES, size)) for c in range(SUBLANES)]
        order = list(range(p + 1, len(blocks))) + list(range(p))
        for q in order:
            total = jnp.where(pivot_lanes, 0.0, blocks[q])
            for c, column in enumerate(columns(blocks[q])):
                total = total - column * spread[c]
            blocks[q] = total
        blocks[p] = row_block
    return jnp.concatenate(blocks, axis=0)


def spread_rows(ref, row):
    ref[...] = jnp.broadcast_to(row.reshape(1, 1, row.shape[-1]), ref.shape)


def diagonal_row(matrix):
    return jnp.sum(jnp.where(eye_mask(matrix.shape[0]), matrix, 0.0), axis=0, keepdims=True)


def solve_kernel(rotates, levels_ref, ham_ref, *refs):
    size = ham_ref.shape[0]
    eye = eye_mask(size)
    level = levels_ref[0]
    for row in range(1, levels_ref.shape[0]):
        level = level + levels_ref[row]
    halved = (0.5 * step_length) * (ham_ref[...] + mean_field * jnp.where(eye, level, 0.0))
    identity = jnp.where(eye, 1.0, 0.0)
    solved = inverse(identity + dot_high(halved, halved))
    unit_real = 2.0 * solved - identity
    unit_imag = -2.0 * dot_high(solved, halved)
    low_real, low_imag = unit_real.astype(jnp.bfloat16), unit_imag.astype(jnp.bfloat16)
    if rotates:
        rho_ref, later_ref, low_ref, unit_ref, left_ref, next_ref = refs
    else:
        low_ref, unit_ref = refs
    low_ref[0:size, 0:size] = low_real
    low_ref[0:size, size:] = low_imag
    low_ref[size:, 0:size] = -low_imag
    low_ref[size:, size:] = low_real
    unit_ref[0] = unit_real
    unit_ref[1] = unit_imag
    if rotates:
        rho_real, rho_imag = rho_ref[0], rho_ref[1]
        left_real = dot_high(unit_real, rho_real) - dot_high(unit_imag, rho_imag)
        left_imag = dot_high(unit_real, rho_imag) + dot_high(unit_imag, rho_real)
        left_ref[0] = left_real
        left_ref[1] = left_imag
        real_diagonal = jnp.sum(left_real * unit_real + left_imag * unit_imag, axis=1, keepdims=True)
        row = jnp.sum(jnp.where(eye, real_diagonal + later_ref[0], 0.0), axis=0, keepdims=True)
        spread_rows(next_ref, row)


IN_VMEM = pl.BlockSpec(memory_space=pltpu.VMEM)
IN_HBM = pl.BlockSpec(memory_space=pl.ANY)


def call(body, outs, args, cost_estimate, scratch=(), scalars=0, streamed=(), streamed_outs=(), grant=8):
    specs = [pl.BlockSpec(memory_space=pltpu.SMEM)] * scalars
    specs += [IN_HBM if i in streamed else IN_VMEM for i in range(scalars, len(args))]
    return pl.pallas_call(
        body,
        out_shape=[
            pltpu.HBM(shape, kind) if i in streamed_outs else jax.ShapeDtypeStruct(shape, kind)
            for i, (shape, kind) in enumerate(outs)
        ],
        in_specs=specs,
        out_specs=[IN_HBM if i in streamed_outs else IN_VMEM for i in range(len(outs))],
        scratch_shapes=list(scratch),
        cost_estimate=cost_estimate,
        compiler_params=pltpu.CompilerParams(vmem_limit_bytes=grant * 2**20 if grant else None),
    )(*args)


def stream(outside, inside, semaphores, base, group, width, inward):
    lanes = lanes_of(base, 0, width)
    ends = (outside.at[:, lanes], inside.at[:, lanes])
    source, target = ends if inward else ends[::-1]
    return pltpu.make_async_copy(source, target, semaphores.at[group])


def solve(levels, hamiltonian, rho=None, later=None):
    size = hamiltonian.shape[0]
    outs = [((2 * size, 2 * size), jnp.bfloat16), ((2, size, size), jnp.float32)]
    args = (levels, hamiltonian)
    if rho is not None:
        outs += [((2, size, size), jnp.float32), (levels.shape, jnp.float32)]
        args += (rho, later)
    estimate = pl.CostEstimate(flops=4_000_000_000, bytes_accessed=1_000_000, transcendentals=0)
    return call(functools.partial(solve_kernel, rho is not None), outs, args, estimate)


def lanes_of(base, first, span):
    return pl.ds(pl.multiple_of(base + first, 128), span)


def sigma_into(sig_ref, row_ref, col_ref, base, rows, span):
    size = sig_ref.shape[0] // 2
    for start in range(0, size, rows):
        for first in range(0, sig_ref.shape[1], span):
            real, imag = pl.ds(start, rows), pl.ds(size + start, rows)
            lanes, here = lanes_of(base, first, span), pl.ds(first, span)
            green_real = row_ref[real, lanes].astype(jnp.float32)
            green_imag = row_ref[imag, lanes].astype(jnp.float32)
            other_real = col_ref[real, lanes].astype(jnp.float32)
            other_imag = col_ref[imag, lanes].astype(jnp.float32)
            square_real = (coupling * coupling) * (green_real * green_real - green_imag * green_imag)
            square_imag = (coupling * coupling * 2.0) * green_real * green_imag
            sig_ref[real, here] = (square_real * other_real - square_imag * other_imag).astype(jnp.bfloat16)
            sig_ref[imag, here] = (square_real * other_imag + square_imag * other_real).astype(jnp.bfloat16)


def overlap(sig, col):
    return lax.dot_general(sig, col, (((1,), (1,)), ((), ())), preferred_element_type=jnp.float32)


def advance_into(out_ref, low, source_ref, base, width, local=False):
    span = min(SPAN, width)
    for first in range(0, width, span):
        lanes = lanes_of(base, first, span)
        target = pl.ds(first, span) if local else lanes
        moved = jnp.dot(low, source_ref[:, lanes], preferred_element_type=jnp.float32)
        out_ref[:, target] = moved.astype(out_ref.dtype)


def row_form(low):
    size = low.shape[0] // 2
    top = jnp.concatenate([low[:size, :size], low[size:, :size]], axis=1)
    bottom = jnp.concatenate([low[:size, size:], low[:size, :size]], axis=1)
    return jnp.concatenate([top, bottom], axis=0)


def each_group(total_width, width, body):
    def step(g, carry):
        body(pl.multiple_of(g * width, width), g)
        return carry

    lax.fori_loop(0, total_width // width, step, 0)


def complex_sum(four):
    size = four.shape[0] // 2
    return four[:size, :size] - four[size:, size:], four[:size, size:] + four[size:, :size]


def finish_sum(acc, before_ref, base_ref, out_ref, scale):
    real, imag = complex_sum(scale * (acc[...] - before_ref[...]))
    if base_ref is not None:
        real, imag = base_ref[0] + real, base_ref[1] + imag
    out_ref[0] = real
    out_ref[1] = imag
    return real


def now_kernel(parts, last, me_ref, row_ref, own_ref, *refs):
    pieces, refs = refs[: parts - 1], refs[parts - 1 :]
    if last:
        before_ref, known_ref, col_hbm, rho_out, level_out, acc, sig, place, col_out, sent = refs
    else:
        col_hbm, acc, sig, place, col_out, sent = refs
    _, count, block, times = pieces[0].shape
    width = sig.shape[1]
    group = width // times
    size = sig.shape[0] // 2
    direct = place.dtype == col_out.dtype
    acc[...] = jnp.zeros_like(acc)

    def body(base, g):
        first = lax.div(base, times)
        for r in range(parts):
            source = lax.bitwise_xor(me_ref[0], r) * block
            for part in range(2):
                rows = pl.ds(pl.multiple_of(part * size + source, block), block)
                for k in range(group):
                    if r == 0:
                        value = own_ref[part, me_ref[0] * count + first + k]
                    else:
                        value = pieces[r - 1][part, first + k]
                    if direct:
                        col_out[rows, lanes_of(base, k * times, times)] = value
                    else:
                        place[rows, pl.ds(k * times, times)] = value.astype(place.dtype)
        if not direct:
            col_out[:, lanes_of(base, 0, width)] = place[...].astype(col_out.dtype)
        stream(col_hbm, col_out, sent, base, g, width, False).start()
        sigma_into(sig, row_ref, col_out, base, 16, min(SPAN, width))
        acc[...] += overlap(sig[...], col_out[:, lanes_of(base, 0, width)])

    each_group(col_out.shape[1], width, body)
    each_group(col_out.shape[1], width, lambda base, g: stream(col_hbm, col_out, sent, base, g, width, False).wait())
    if last:
        real = finish_sum(acc, before_ref, known_ref, rho_out, step_length)
        spread_rows(level_out, diagonal_row(real))


def later_kernel(last, row_hbm, col_hbm, low_ref, *refs):
    if last:
        before_ref, row_to, col_to, sum_out, acc, *refs = refs
    else:
        row_to, col_to, acc, *refs = refs
    sig, row_ref, col_ref, row_out, col_out, row_came, col_came, row_went, col_went = refs
    total_width, width = row_ref.shape[1], sig.shape[1]

    def loads(base, g):
        return (
            stream(row_hbm, row_ref, row_came, base, g, width, True),
            stream(col_hbm, col_ref, col_came, base, g, width, True),
        )

    def stores(base, g):
        return (
            stream(row_to, row_out, row_went, base, g, width, False),
            stream(col_to, col_out, col_went, base, g, width, False),
        )

    def start(base, g):
        for copy in loads(base, g):
            copy.start()

    def wait(base, g):
        for copy in stores(base, g):
            copy.wait()

    each_group(total_width, width, start)
    acc[...] = jnp.zeros_like(acc)

    def body(base, g):
        for copy in loads(base, g):
            copy.wait()
        advance_into(row_out, row_form(low_ref[...]), row_ref, base, width)
        advance_into(col_out, low_ref[...], col_ref, base, width)
        for copy in stores(base, g):
            copy.start()
        sigma_into(sig, row_out, col_out, base, 16, min(SPAN, width))
        acc[...] += overlap(sig[...], col_out[:, lanes_of(base, 0, width)])

    each_group(total_width, width, body)
    if last:
        finish_sum(acc, before_ref, None, sum_out, step_length)
    each_group(total_width, width, wait)


def finish_kernel(left_ref, unit_ref, later_ref, unit_last_ref, last_ref, rho_ref):
    def right(real, imag, unit):
        turned_real, turned_imag = unit[0].T, unit[1].T
        return (
            dot_high(real, turned_real) + dot_high(imag, turned_imag),
            dot_high(imag, turned_real) - dot_high(real, turned_imag),
        )

    real, imag = right(left_ref[0], left_ref[1], unit_ref)
    real, imag = real + later_ref[0], imag + later_ref[1]
    unit_real, unit_imag = unit_last_ref[0], unit_last_ref[1]
    left_real = dot_high(unit_real, real) - dot_high(unit_imag, imag)
    left_imag = dot_high(unit_real, imag) + dot_high(unit_imag, real)
    real, imag = right(left_real, left_imag, unit_last_ref)
    rho_ref[0] = real + last_ref[0]
    rho_ref[1] = imag + last_ref[1]


def row_kernel(width, row_ref, low_ref, row_out):
    low = row_form(low_ref[...])
    each_group(row_ref.shape[1], width, lambda base, g: advance_into(row_out, low, row_ref, base, width))


def ready_kernel(parts, me_ref, col_ref, own_ref, *refs):
    pieces, (low_first_ref, low_ref, out_ref, place, moved) = refs[: parts - 1], refs[parts - 1 :]
    _, mirrored, block, times = pieces[0].shape
    size, width = place.shape[0] // 2, place.shape[1]
    own_width = col_ref.shape[1]
    each_group(own_width, width, lambda base, g: advance_into(out_ref, low_ref[...], col_ref, base, width))
    far = lax.bitwise_xor(me_ref[0], parts // 2) * (size // parts)
    for r in range(parts):
        source = lax.bitwise_xor(me_ref[0], r) * block
        for part in range(2):
            rows = pl.ds(pl.multiple_of(part * size + source, block), block)
            for k in range(mirrored):
                value = own_ref[part, far + k] if r == 0 else pieces[r - 1][part, k]
                place[rows, pl.ds(k * times, times)] = value.astype(place.dtype)
    span = min(SPAN, width)
    for first in range(0, width, span):
        lanes = pl.ds(first, span)
        once = jnp.dot(low_first_ref[...], place[:, lanes].astype(jnp.bfloat16), preferred_element_type=jnp.float32)
        moved[:, lanes] = once.astype(moved.dtype)
        twice = jnp.dot(low_ref[...], moved[:, lanes], preferred_element_type=jnp.float32)
        out_ref[:, pl.ds(own_width + first, span)] = twice.astype(out_ref.dtype)


def last_kernel(parts, me_ref, col_ref, low_ref, *refs):
    outs, moved = refs[:parts], refs[parts]
    _, rows_near, block, times = outs[0].shape
    width = moved.shape[1]
    size = moved.shape[0] // 2
    group = width // times
    count = rows_near - group
    low = low_ref[...]

    def body(base, g):
        first = lax.div(base, times)
        advance_into(moved, low, col_ref, base, width, local=True)

        def cut(r, offset):
            target = lax.bitwise_xor(me_ref[0], r) * block
            for part in range(2):
                rows = pl.ds(pl.multiple_of(part * size + target, block), block)
                for k in range(group):
                    outs[r][part, first + (k - offset)] = moved[rows, pl.ds(k * times, times)].astype(outs[r].dtype)

        for r in range(parts // 2):
            cut(r, 0)

        @pl.when((first >= group) & (first < count))
        def _():
            for r in range(parts // 2, parts):
                cut(r, group)

    each_group(col_ref.shape[1], width, body)


def cost(arrays, products):
    return pl.CostEstimate(flops=products * 2 * 256 * 256 * 4096, bytes_accessed=arrays * 2**21, transcendentals=0)


def place_type(block):
    return jnp.bfloat16 if block % 16 == 0 else jnp.float32


def sum_scratch(size, width):
    return [pltpu.VMEM((2 * size, 2 * size), jnp.float32), pltpu.VMEM((2 * size, width), jnp.bfloat16)]


def now_step(me, row, own, pieces, before=None, known=None, devices=0):
    size = own.shape[1]
    _, count, block, times = pieces[0].shape
    width = min(GROUP, count) * times
    square, history = ((2 * size, 2 * size), jnp.float32), (row.shape, jnp.bfloat16)
    args = (me, row, own, *pieces)
    scratch = sum_scratch(size, width)
    scratch += [pltpu.VMEM((2 * size, width), place_type(block)), pltpu.VMEM(row.shape, jnp.bfloat16)]
    scratch += [pltpu.SemaphoreType.DMA((row.shape[1] // width,))]
    body = functools.partial(now_kernel, len(pieces) + 1, before is not None)
    if before is None:
        outs, scratch = [history, square], scratch[1:]
    else:
        outs, args = [history, ((2, size, size), jnp.float32), ((devices, 1, size), jnp.float32)], args + (before, known)
    return call(body, outs, args, cost(4, 2), scratch, 1, streamed_outs=(0,))


def later_step(row, col, low, width, before=None):
    double = row.shape[0]
    square, history = ((double, double), jnp.float32), (row.shape, jnp.bfloat16)
    body = functools.partial(later_kernel, before is not None)
    scratch = sum_scratch(double // 2, width) + [pltpu.VMEM(row.shape, jnp.bfloat16)] * 4
    scratch += [pltpu.SemaphoreType.DMA((row.shape[1] // width,))] * 4
    if before is None:
        outs, args, scratch = [history, history, square], (row, col, low), scratch[1:]
    else:
        outs, args = [history, history, ((2, double // 2, double // 2), jnp.float32)], (row, col, low, before)
    return call(body, outs, args, cost(4, 3), scratch, 0, (0, 1), (0, 1), None)


def row_step(row, low, width):
    body = functools.partial(row_kernel, width)
    return call(body, [(row.shape, jnp.bfloat16)], (row, low), cost(2, 1))[0]


def ready_step(me, col, own, pieces, low_first, low):
    double = col.shape[0]
    _, mirrored, block, times = pieces[0].shape
    width = mirrored * times
    out = ((double, col.shape[1] + width), jnp.bfloat16)
    scratch = [pltpu.VMEM((double, width), place_type(block)), pltpu.VMEM((double, width), jnp.bfloat16)]
    body = functools.partial(ready_kernel, len(pieces) + 1)
    return call(body, [out], (me, col, own, *pieces, low_first, low), cost(3, 1), scratch, 1)[0]


def last_step(me, ready, low, parts, mirrored, times):
    double = ready.shape[0]
    block = double // 2 // parts
    count = ready.shape[1] // times - mirrored
    near = ((2, count + mirrored, block, times), jnp.bfloat16)
    far = ((2, count - mirrored, block, times), jnp.bfloat16)
    outs = [near] * (parts // 2) + [far] * (parts - parts // 2)
    scratch = [pltpu.VMEM((double, mirrored * times), place_type(block))]
    body = functools.partial(last_kernel, parts)
    return call(body, outs, (me, ready, low), cost(2, 1), scratch, 1)


def tree_sum(values):
    while len(values) > 1:
        values = [values[i] + values[i + 1] for i in range(0, len(values), 2)]
    return values[0]


def swap(value, name, r):
    return lax.ppermute(value, name, [(j, j ^ r) for j in range(lax.axis_size(name))])


def part_total(values):
    count = lax.axis_size("hist")
    rows = values.reshape(count, -1, values.shape[-1])
    share = jnp.sum(lax.all_to_all(rows, "hist", 0, 0, tiled=True), axis=0)
    return share


def whole_total(share, shape):
    count = lax.axis_size("hist")
    moved = [share]
    for r in range(1, lax.axis_size("col")):
        moved.append(swap(share, "col", r))
    share = tree_sum(moved)
    return lax.all_to_all(jnp.broadcast_to(share, (count,) + share.shape), "hist", 0, 0, tiled=True).reshape(shape)


def finish_rotation(left, unit):
    high = functools.partial(jnp.dot, precision=HIGH)
    real = high(left[0], unit[0].T) + high(left[1], unit[1].T)
    imag = high(left[1], unit[0].T) - high(left[0], unit[1].T)
    return jnp.stack([real, imag])


def rotate(unit, rho):
    high = functools.partial(jnp.dot, precision=HIGH)
    real = high(unit[0], rho[0]) - high(unit[1], rho[1])
    imag = high(unit[0], rho[1]) + high(unit[1], rho[0])
    return finish_rotation((real, imag), unit)


def gather_pieces(col):
    me, parts = lax.axis_index("col"), lax.axis_size("col")
    count = col.shape[1] // parts
    pieces = []
    for r in range(1, parts):
        piece = lax.dynamic_slice_in_dim(col, (me ^ r) * count, count, axis=1)
        pieces.append(swap(piece, "col", r))
    return pieces


def mirror_slices(col, mirrored):
    me, parts = lax.axis_index("col"), lax.axis_size("col")
    count = col.shape[1] // parts
    starts = [(me ^ r ^ (parts // 2)) * count for r in range(1, parts)]
    return [lax.dynamic_slice_in_dim(col, start, mirrored, axis=1) for start in starts]


def mirror_pieces(slices):
    pieces = []
    for r, piece in enumerate(slices, 1):
        pieces.append(swap(piece, "col", r))
    return pieces


def return_pieces(pieces):
    me, parts = lax.axis_index("col"), lax.axis_size("col")
    _, near, block, times = pieces[0].shape
    mirrored = (near - pieces[-1].shape[1]) // 2
    count = near - mirrored
    out = jnp.zeros((2, parts * count, block, times), pieces[0].dtype)
    for r, piece in enumerate(pieces):
        moved = piece if r == 0 else swap(piece, "col", r)
        if r < parts // 2:
            out = lax.dynamic_update_slice_in_dim(out, moved[:, :count], (me ^ r) * count, axis=1)
            out = lax.dynamic_update_slice_in_dim(out, moved[:, count:], (me ^ r ^ (parts // 2)) * count, axis=1)
        else:
            out = lax.dynamic_update_slice_in_dim(out, moved, (me ^ r) * count + mirrored, axis=1)
    return out


def per_device(less_row, less_col, great_row, great_col, density, hamiltonian):
    size, count, times = less_row.shape[1:]
    parts = lax.axis_size("col")
    devices = parts * lax.axis_size("hist")
    me = lax.axis_index("col").astype(jnp.int32).reshape(1)
    width = min(GROUP, count) * times
    mirrored = count // 4

    great_pieces = gather_pieces(great_col)
    less_pieces = gather_pieces(less_col)
    great_slices = mirror_slices(great_col, mirrored)
    less_slices = mirror_slices(less_col, mirrored)

    symmetric = 0.5 * (hamiltonian + hamiltonian.T)
    low_first, unit = solve(diagonal_row(density[0]).reshape(1, 1, size), symmetric)
    known = rotate(unit, density * (1.0 / devices))

    less = less_row.reshape(2 * size, count * times)
    great = great_row.reshape(2 * size, count * times)
    cols_great, minus = now_step(me, less, great_col, great_pieces)
    less, cols_great, minus_later = later_step(less, cols_great, low_first, width)
    less_pieces, minus_later = lax.optimization_barrier((less_pieces, minus_later))
    great_slices, _ = lax.optimization_barrier((great_slices, less_pieces[0]))
    great_far = mirror_pieces(great_slices)
    cols_less, rho, part = now_step(me, great, less_col, less_pieces, minus, known, devices)

    levels = lax.all_to_all(part, ("hist", "col"), 0, 0, tiled=True)
    great, cols_less, later = later_step(great, cols_less, low_first, width, minus_later)
    low, unit, left, part = solve(levels, symmetric, rho, later)

    levels = lax.all_to_all(part, ("hist", "col"), 0, 0, tiled=True)
    less_slices, _ = lax.optimization_barrier((less_slices, part))
    less_far = mirror_pieces(less_slices)
    great_ready = ready_step(me, cols_great, great_col, great_far, low_first, low)
    low_last, unit_last = solve(levels, symmetric)

    great_out = return_pieces(last_step(me, great_ready, low_last, parts, mirrored, times))
    less, _, minus = later_step(less, cols_great, low, width)
    great, _, last = later_step(great, cols_less, low, width, minus)
    args = (left, unit, later, unit_last, last)
    estimate = pl.CostEstimate(flops=500_000_000, bytes_accessed=1_000_000, transcendentals=0)
    rho = call(finish_kernel, [(density.shape, jnp.float32)], args, estimate)[0]
    share = part_total(rho)
    less_ready = ready_step(me, cols_less, less_col, less_far, low_first, low)
    less_ready, share = lax.optimization_barrier((less_ready, share))
    less_out = return_pieces(last_step(me, less_ready, low_last, parts, mirrored, times))
    rho = whole_total(share, density.shape)
    less_row_out = row_step(less, low_last, width).reshape(less_row.shape)
    great_row_out = row_step(great, low_last, width).reshape(great_row.shape)
    return (less_row_out, less_out, great_row_out, great_out, rho)


def solution(mesh):
    history = P(None, None, "col", "hist")
    return jax.shard_map(
        per_device,
        mesh=mesh,
        in_specs=(history, history, history, history, P(), P()),
        out_specs=(history, history, history, history, P()),
        check_vma=False,
    )
```

```python
import functools

import jax
import jax.numpy as jnp
from jax import lax
from jax.experimental import pallas as pl
from jax.experimental.pallas import tpu as pltpu
from jax.sharding import PartitionSpec as P


step_length = 0.1
mean_field = 2.0
coupling = 1.0

HIGH = lax.Precision.HIGHEST
SUBLANES = 8
GROUP = 8
SPAN = 256


def dot_high(a, b):
    return jnp.dot(a, b, precision=HIGH, preferred_element_type=jnp.float32)


def eye_mask(size):
    rows = lax.broadcasted_iota(jnp.int32, (size, size), 0)
    return rows == lax.broadcasted_iota(jnp.int32, (size, size), 1)


def inverse(matrix):
    size = matrix.shape[0]
    blocks = [matrix[p : p + SUBLANES] for p in range(0, size, SUBLANES)]
    rows = lax.broadcasted_iota(jnp.int32, (SUBLANES, size), 0)
    lanes = lax.broadcasted_iota(jnp.int32, (SUBLANES, size), 1)
    for p in range(len(blocks)):
        first = p * SUBLANES
        pivot_lanes = (lanes >= first) & (lanes < first + SUBLANES)

        def columns(block):
            return [jnp.broadcast_to(block[:, first + c : first + c + 1], (SUBLANES, size)) for c in range(SUBLANES)]

        pivot = columns(blocks[p])
        row_block = jnp.where(pivot_lanes, jnp.where(lanes == rows + first, 1.0, 0.0), blocks[p])
        for j in range(SUBLANES):

            def across(value):
                return jnp.broadcast_to(value[j : j + 1], (SUBLANES, size))

            scale = 1.0 / across(pivot[j])
            factor = pivot[j]

            def eliminate(value):
                top = across(value) * scale
                return jnp.where(rows == j, top, value - factor * top)

            row_block = eliminate(row_block)
            pivot = [eliminate(value) if c > j else value for c, value in enumerate(pivot)]
        spread = [jnp.broadcast_to(row_block[c : c + 1], (SUBLANES, size)) for c in range(SUBLANES)]
        order = list(range(p + 1, len(blocks))) + list(range(p))
        for q in order:
            total = jnp.where(pivot_lanes, 0.0, blocks[q])
            for c, column in enumerate(columns(blocks[q])):
                total = total - column * spread[c]
            blocks[q] = total
        blocks[p] = row_block
    return jnp.concatenate(blocks, axis=0)


def spread_rows(ref, row):
    ref[...] = jnp.broadcast_to(row.reshape(1, 1, row.shape[-1]), ref.shape)


def diagonal_row(matrix):
    return jnp.sum(jnp.where(eye_mask(matrix.shape[0]), matrix, 0.0), axis=0, keepdims=True)


def solve_kernel(rotates, levels_ref, ham_ref, *refs):
    size = ham_ref.shape[0]
    eye = eye_mask(size)
    level = levels_ref[0]
    for row in range(1, levels_ref.shape[0]):
        level = level + levels_ref[row]
    halved = (0.5 * step_length) * (ham_ref[...] + mean_field * jnp.where(eye, level, 0.0))
    identity = jnp.where(eye, 1.0, 0.0)
    solved = inverse(identity + dot_high(halved, halved))
    unit_real = 2.0 * solved - identity
    unit_imag = -2.0 * dot_high(solved, halved)
    low_real, low_imag = unit_real.astype(jnp.bfloat16), unit_imag.astype(jnp.bfloat16)
    if rotates:
        rho_ref, later_ref, low_ref, unit_ref, left_ref, next_ref = refs
    else:
        low_ref, unit_ref = refs
    low_ref[0:size, 0:size] = low_real
    low_ref[0:size, size:] = low_imag
    low_ref[size:, 0:size] = -low_imag
    low_ref[size:, size:] = low_real
    unit_ref[0] = unit_real
    unit_ref[1] = unit_imag
    if rotates:
        rho_real, rho_imag = rho_ref[0], rho_ref[1]
        left_real = dot_high(unit_real, rho_real) - dot_high(unit_imag, rho_imag)
        left_imag = dot_high(unit_real, rho_imag) + dot_high(unit_imag, rho_real)
        left_ref[0] = left_real
        left_ref[1] = left_imag
        real_diagonal = jnp.sum(left_real * unit_real + left_imag * unit_imag, axis=1, keepdims=True)
        row = jnp.sum(jnp.where(eye, real_diagonal + later_ref[0], 0.0), axis=0, keepdims=True)
        spread_rows(next_ref, row)


IN_VMEM = pl.BlockSpec(memory_space=pltpu.VMEM)
IN_HBM = pl.BlockSpec(memory_space=pl.ANY)


def call(body, outs, args, cost_estimate, scratch=(), scalars=0, streamed=(), streamed_outs=(), grant=8):
    specs = [pl.BlockSpec(memory_space=pltpu.SMEM)] * scalars
    specs += [IN_HBM if i in streamed else IN_VMEM for i in range(scalars, len(args))]
    return pl.pallas_call(
        body,
        out_shape=[
            pltpu.HBM(shape, kind) if i in streamed_outs else jax.ShapeDtypeStruct(shape, kind)
            for i, (shape, kind) in enumerate(outs)
        ],
        in_specs=specs,
        out_specs=[IN_HBM if i in streamed_outs else IN_VMEM for i in range(len(outs))],
        scratch_shapes=list(scratch),
        cost_estimate=cost_estimate,
        compiler_params=pltpu.CompilerParams(vmem_limit_bytes=grant * 2**20 if grant else None),
    )(*args)


def stream(outside, inside, semaphores, base, group, width, inward):
    lanes = lanes_of(base, 0, width)
    ends = (outside.at[:, lanes], inside.at[:, lanes])
    source, target = ends if inward else ends[::-1]
    return pltpu.make_async_copy(source, target, semaphores.at[group])


def solve(levels, hamiltonian, rho=None, later=None):
    size = hamiltonian.shape[0]
    outs = [((2 * size, 2 * size), jnp.bfloat16), ((2, size, size), jnp.float32)]
    args = (levels, hamiltonian)
    if rho is not None:
        outs += [((2, size, size), jnp.float32), (levels.shape, jnp.float32)]
        args += (rho, later)
    estimate = pl.CostEstimate(flops=4_000_000_000, bytes_accessed=1_000_000, transcendentals=0)
    return call(functools.partial(solve_kernel, rho is not None), outs, args, estimate)


def lanes_of(base, first, span):
    return pl.ds(pl.multiple_of(base + first, 128), span)


def sigma_into(sig_ref, row_ref, col_ref, base, rows, span):
    size = sig_ref.shape[0] // 2
    for start in range(0, size, rows):
        for first in range(0, sig_ref.shape[1], span):
            real, imag = pl.ds(start, rows), pl.ds(size + start, rows)
            lanes, here = lanes_of(base, first, span), pl.ds(first, span)
            green_real = row_ref[real, lanes].astype(jnp.float32)
            green_imag = row_ref[imag, lanes].astype(jnp.float32)
            other_real = col_ref[real, lanes].astype(jnp.float32)
            other_imag = col_ref[imag, lanes].astype(jnp.float32)
            square_real = (coupling * coupling) * (green_real * green_real - green_imag * green_imag)
            square_imag = (coupling * coupling * 2.0) * green_real * green_imag
            sig_ref[real, here] = (square_real * other_real - square_imag * other_imag).astype(jnp.bfloat16)
            sig_ref[imag, here] = (square_real * other_imag + square_imag * other_real).astype(jnp.bfloat16)


def overlap(sig, col):
    return lax.dot_general(sig, col, (((1,), (1,)), ((), ())), preferred_element_type=jnp.float32)


def advance_into(out_ref, low, source_ref, base, width, local=False):
    span = min(SPAN, width)
    for first in range(0, width, span):
        lanes = lanes_of(base, first, span)
        target = pl.ds(first, span) if local else lanes
        moved = jnp.dot(low, source_ref[:, lanes], preferred_element_type=jnp.float32)
        out_ref[:, target] = moved.astype(out_ref.dtype)


def row_form(low):
    size = low.shape[0] // 2
    top = jnp.concatenate([low[:size, :size], low[size:, :size]], axis=1)
    bottom = jnp.concatenate([low[:size, size:], low[:size, :size]], axis=1)
    return jnp.concatenate([top, bottom], axis=0)


def each_group(total_width, width, body):
    def step(g, carry):
        body(pl.multiple_of(g * width, width), g)
        return carry

    lax.fori_loop(0, total_width // width, step, 0)


def complex_sum(four):
    size = four.shape[0] // 2
    return four[:size, :size] - four[size:, size:], four[:size, size:] + four[size:, :size]


def finish_sum(acc, before_ref, base_ref, out_ref, scale):
    real, imag = complex_sum(scale * (acc[...] - before_ref[...]))
    if base_ref is not None:
        real, imag = base_ref[0] + real, base_ref[1] + imag
    out_ref[0] = real
    out_ref[1] = imag
    return real


def now_kernel(parts, last, me_ref, row_hbm, *refs):
    pieces, refs = refs[:parts], refs[parts:]
    if last:
        before_ref, known_ref, col_hbm, rho_out, level_out, acc, *refs = refs
    else:
        col_hbm, acc, *refs = refs
    sig, place, col_out, row_ref, held, sent, row_came, came = refs
    _, _, _, block, times = held.shape
    total_width, width = col_out.shape[1], sig.shape[1]
    group = width // times
    size = sig.shape[0] // 2
    direct = place.dtype == col_out.dtype
    arrivals = [pltpu.make_async_copy(pieces[r], held.at[r], came.at[r]) for r in range(parts)]
    for copy in arrivals:
        copy.start()
    each_group(total_width, width, lambda base, g: stream(row_hbm, row_ref, row_came, base, g, width, True).start())
    acc[...] = jnp.zeros_like(acc)
    for copy in arrivals:
        copy.wait()

    def body(base, g):
        first = lax.div(base, times)
        for r in range(parts):
            source = lax.bitwise_xor(me_ref[0], r) * block
            for part in range(2):
                rows = pl.ds(pl.multiple_of(part * size + source, block), block)
                for k in range(group):
                    value = held[r, part, first + k]
                    if direct:
                        col_out[rows, lanes_of(base, k * times, times)] = value
                    else:
                        place[rows, pl.ds(k * times, times)] = value.astype(place.dtype)
        if not direct:
            col_out[:, lanes_of(base, 0, width)] = place[...].astype(col_out.dtype)
        stream(col_hbm, col_out, sent, base, g, width, False).start()
        stream(row_hbm, row_ref, row_came, base, g, width, True).wait()
        sigma_into(sig, row_ref, col_out, base, 16, min(SPAN, width))
        acc[...] += overlap(sig[...], col_out[:, lanes_of(base, 0, width)])

    each_group(total_width, width, body)
    if last:
        real = finish_sum(acc, before_ref, known_ref, rho_out, step_length)
        spread_rows(level_out, diagonal_row(real))
    each_group(total_width, width, lambda base, g: stream(col_hbm, col_out, sent, base, g, width, False).wait())


def later_kernel(last, row_hbm, col_hbm, low_ref, *refs):
    if last:
        before_ref, row_to, col_to, sum_out, acc, *refs = refs
    else:
        row_to, col_to, acc, *refs = refs
    sig, row_ref, col_ref, row_out, col_out, row_came, col_came, row_went, col_went = refs
    total_width, width = row_ref.shape[1], sig.shape[1]

    def loads(base, g):
        return (
            stream(row_hbm, row_ref, row_came, base, g, width, True),
            stream(col_hbm, col_ref, col_came, base, g, width, True),
        )

    def stores(base, g):
        return (
            stream(row_to, row_out, row_went, base, g, width, False),
            stream(col_to, col_out, col_went, base, g, width, False),
        )

    def start(base, g):
        for copy in loads(base, g):
            copy.start()

    def wait(base, g):
        for copy in stores(base, g):
            copy.wait()

    each_group(total_width, width, start)
    acc[...] = jnp.zeros_like(acc)

    def body(base, g):
        for copy in loads(base, g):
            copy.wait()
        advance_into(row_out, row_form(low_ref[...]), row_ref, base, width)
        advance_into(col_out, low_ref[...], col_ref, base, width)
        for copy in stores(base, g):
            copy.start()
        sigma_into(sig, row_out, col_out, base, 16, min(SPAN, width))
        acc[...] += overlap(sig[...], col_out[:, lanes_of(base, 0, width)])

    each_group(total_width, width, body)
    if last:
        finish_sum(acc, before_ref, None, sum_out, step_length)
    each_group(total_width, width, wait)


def finish_kernel(left_ref, unit_ref, later_ref, unit_last_ref, last_ref, rho_ref):
    def right(real, imag, unit):
        turned_real, turned_imag = unit[0].T, unit[1].T
        return (
            dot_high(real, turned_real) + dot_high(imag, turned_imag),
            dot_high(imag, turned_real) - dot_high(real, turned_imag),
        )

    real, imag = right(left_ref[0], left_ref[1], unit_ref)
    real, imag = real + later_ref[0], imag + later_ref[1]
    unit_real, unit_imag = unit_last_ref[0], unit_last_ref[1]
    left_real = dot_high(unit_real, real) - dot_high(unit_imag, imag)
    left_imag = dot_high(unit_real, imag) + dot_high(unit_imag, real)
    real, imag = right(left_real, left_imag, unit_last_ref)
    rho_ref[0] = real + last_ref[0]
    rho_ref[1] = imag + last_ref[1]


def row_kernel(width, row_ref, low_ref, row_out):
    low = row_form(low_ref[...])
    each_group(row_ref.shape[1], width, lambda base, g: advance_into(row_out, low, row_ref, base, width))


def last_kernel(parts, me_ref, col_ref, low_first_ref, low_ref, low_last_ref, *refs):
    pieces, outs, (place, once, moved) = refs[:parts], refs[parts : 2 * parts], refs[2 * parts :]
    _, mirrored, block, times = pieces[0].shape
    size, width = moved.shape[0] // 2, moved.shape[1]
    count = col_ref.shape[1] // times

    def advance(out_ref, low, source_ref, base):
        span = min(SPAN, width)
        for first in range(0, width, span):
            source = source_ref[:, lanes_of(base, first, span)].astype(jnp.bfloat16)
            after = jnp.dot(low[...], source, preferred_element_type=jnp.float32)
            out_ref[:, pl.ds(first, span)] = after.astype(jnp.bfloat16).astype(out_ref.dtype)

    def cut(r, to):
        target = lax.bitwise_xor(me_ref[0], r) * block
        for part in range(2):
            rows = pl.ds(pl.multiple_of(part * size + target, block), block)
            for k in range(mirrored):
                outs[r][part, to + k] = moved[rows, pl.ds(k * times, times)].astype(outs[r].dtype)

    def body(base, g):
        first = lax.div(base, times)
        advance(once, low_ref, col_ref, base)
        advance(moved, low_last_ref, once, 0)
        for r in range(parts // 2):
            cut(r, first)

        @pl.when(first >= mirrored)
        def _():
            for r in range(parts // 2, parts):
                cut(r, first - mirrored)

    each_group(count * times, width, body)
    for r in range(parts):
        source = lax.bitwise_xor(me_ref[0], r) * block
        for part in range(2):
            rows = pl.ds(pl.multiple_of(part * size + source, block), block)
            for k in range(mirrored):
                place[rows, pl.ds(k * times, times)] = pieces[r][part, k].astype(place.dtype)
    advance(once, low_first_ref, place, 0)
    advance(place, low_ref, once, 0)
    advance(moved, low_last_ref, place, 0)
    for r in range(parts // 2):
        cut(r, count)


def cost(arrays, products):
    return pl.CostEstimate(flops=products * 2 * 256 * 256 * 4096, bytes_accessed=arrays * 2**21, transcendentals=0)


def place_type(block):
    return jnp.bfloat16 if block % 16 == 0 else jnp.float32


def sum_scratch(size, width):
    return [pltpu.VMEM((2 * size, 2 * size), jnp.float32), pltpu.VMEM((2 * size, width), jnp.bfloat16)]


def now_step(me, row, pieces, before=None, known=None, devices=0):
    parts = len(pieces)
    _, count, block, times = pieces[0].shape
    size = parts * block
    width = min(GROUP, count) * times
    groups = row.shape[1] // width
    square, history = ((2 * size, 2 * size), jnp.float32), (row.shape, jnp.bfloat16)
    args = (me, row, *pieces)
    scratch = sum_scratch(size, width)
    scratch += [pltpu.VMEM((2 * size, width), place_type(block))] + [pltpu.VMEM(row.shape, jnp.bfloat16)] * 2
    scratch += [pltpu.VMEM((parts,) + pieces[0].shape, jnp.bfloat16)]
    scratch += [pltpu.SemaphoreType.DMA((groups,))] * 2 + [pltpu.SemaphoreType.DMA((parts,))]
    body = functools.partial(now_kernel, parts, before is not None)
    if before is None:
        outs, scratch = [history, square], scratch[1:]
    else:
        outs, args = [history, ((2, size, size), jnp.float32), ((devices, 1, size), jnp.float32)], args + (before, known)
    return call(body, outs, args, cost(4, 2), scratch, 1, range(1, parts + 2), (0,), None)


def later_step(row, col, low, width, before=None):
    double = row.shape[0]
    square, history = ((double, double), jnp.float32), (row.shape, jnp.bfloat16)
    body = functools.partial(later_kernel, before is not None)
    scratch = sum_scratch(double // 2, width) + [pltpu.VMEM(row.shape, jnp.bfloat16)] * 4
    scratch += [pltpu.SemaphoreType.DMA((row.shape[1] // width,))] * 4
    if before is None:
        outs, args, scratch = [history, history, square], (row, col, low), scratch[1:]
    else:
        outs, args = [history, history, ((2, double // 2, double // 2), jnp.float32)], (row, col, low, before)
    return call(body, outs, args, cost(4, 3), scratch, 0, (0, 1), (0, 1), None)


def row_step(row, low, width):
    body = functools.partial(row_kernel, width)
    return call(body, [(row.shape, jnp.bfloat16)], (row, low), cost(2, 1))[0]


def last_step(me, col, pieces, low_first, low, low_last):
    double, parts = col.shape[0], len(pieces)
    _, mirrored, block, times = pieces[0].shape
    count = col.shape[1] // times
    near = ((2, count + mirrored, block, times), jnp.bfloat16)
    far = ((2, count - mirrored, block, times), jnp.bfloat16)
    outs = [near] * (parts // 2) + [far] * (parts - parts // 2)
    kind = place_type(block)
    scratch = [pltpu.VMEM((double, mirrored * times), k) for k in (kind, jnp.bfloat16, kind)]
    body = functools.partial(last_kernel, parts)
    return call(body, outs, (me, col, low_first, low, low_last, *pieces), cost(3, 2), scratch, 1)


def tree_sum(values):
    while len(values) > 1:
        values = [values[i] + values[i + 1] for i in range(0, len(values), 2)]
    return values[0]


def swap(value, name, r):
    return lax.ppermute(value, name, [(j, j ^ r) for j in range(lax.axis_size(name))])


def part_total(values):
    count = lax.axis_size("hist")
    rows = values.reshape(count, -1, values.shape[-1])
    share = jnp.sum(lax.all_to_all(rows, "hist", 0, 0, tiled=True), axis=0)
    return share


def whole_total(share, shape):
    count = lax.axis_size("hist")
    moved = [share]
    for r in range(1, lax.axis_size("col")):
        moved.append(swap(share, "col", r))
    share = tree_sum(moved)
    return lax.all_to_all(jnp.broadcast_to(share, (count,) + share.shape), "hist", 0, 0, tiled=True).reshape(shape)


def finish_rotation(left, unit):
    high = functools.partial(jnp.dot, precision=HIGH)
    real = high(left[0], unit[0].T) + high(left[1], unit[1].T)
    imag = high(left[1], unit[0].T) - high(left[0], unit[1].T)
    return jnp.stack([real, imag])


def rotate(unit, rho):
    high = functools.partial(jnp.dot, precision=HIGH)
    real = high(unit[0], rho[0]) - high(unit[1], rho[1])
    imag = high(unit[0], rho[1]) + high(unit[1], rho[0])
    return finish_rotation((real, imag), unit)


def gather_pieces(col):
    me, parts = lax.axis_index("col"), lax.axis_size("col")
    count = col.shape[1] // parts
    pieces = []
    for r in range(parts):
        piece = lax.dynamic_slice_in_dim(col, (me ^ r) * count, count, axis=1)
        pieces.append(swap(piece, "col", r) if r else piece)
    return pieces


def mirror_slices(col, mirrored):
    me, parts = lax.axis_index("col"), lax.axis_size("col")
    count = col.shape[1] // parts
    starts = [(me ^ r ^ (parts // 2)) * count for r in range(parts)]
    return [lax.dynamic_slice_in_dim(col, start, mirrored, axis=1) for start in starts]


def mirror_pieces(slices):
    pieces = []
    for r, piece in enumerate(slices):
        pieces.append(swap(piece, "col", r) if r else piece)
    return pieces


def return_pieces(pieces):
    me, parts = lax.axis_index("col"), lax.axis_size("col")
    _, near, block, times = pieces[0].shape
    mirrored = (near - pieces[-1].shape[1]) // 2
    count = near - mirrored
    out = jnp.zeros((2, parts * count, block, times), pieces[0].dtype)
    half = parts // 2
    for r in [half, 0] + [r for r in range(1, parts) if r != half]:
        moved = pieces[r] if r == 0 else swap(pieces[r], "col", r)
        if r < half:
            out = lax.dynamic_update_slice_in_dim(out, moved[:, :count], (me ^ r) * count, axis=1)
            out = lax.dynamic_update_slice_in_dim(out, moved[:, count:], (me ^ r ^ half) * count, axis=1)
        else:
            out = lax.dynamic_update_slice_in_dim(out, moved, (me ^ r) * count + mirrored, axis=1)
    return out


def per_device(less_row, less_col, great_row, great_col, density, hamiltonian):
    size, count, times = less_row.shape[1:]
    parts = lax.axis_size("col")
    devices = parts * lax.axis_size("hist")
    me = lax.axis_index("col").astype(jnp.int32).reshape(1)
    width = min(GROUP, count) * times
    mirrored = count // 4

    great_pieces = gather_pieces(great_col)
    less_pieces = gather_pieces(less_col)
    far_slices = (mirror_slices(great_col, mirrored), mirror_slices(less_col, mirrored))

    symmetric = 0.5 * (hamiltonian + hamiltonian.T)
    low_first, unit = solve(diagonal_row(density[0]).reshape(1, 1, size), symmetric)
    known = rotate(unit, density * (1.0 / devices))

    less = less_row.reshape(2 * size, count * times)
    great = great_row.reshape(2 * size, count * times)
    cols_great, minus = now_step(me, less, great_pieces)
    less, cols_great, minus_later = later_step(less, cols_great, low_first, width)
    less_pieces, far_slices, minus_later = lax.optimization_barrier((less_pieces, far_slices, minus_later))
    cols_less, rho, part = now_step(me, great, less_pieces, minus, known, devices)

    levels = lax.all_to_all(part, ("hist", "col"), 0, 0, tiled=True)
    great, cols_less, later = later_step(great, cols_less, low_first, width, minus_later)
    low, unit, left, part = solve(levels, symmetric, rho, later)

    levels = lax.all_to_all(part, ("hist", "col"), 0, 0, tiled=True)
    far_slices, _ = lax.optimization_barrier((far_slices, part))
    great_far = mirror_pieces(far_slices[0])
    less_far = mirror_pieces(far_slices[1])
    low_last, unit_last = solve(levels, symmetric)

    great_out = return_pieces(last_step(me, cols_great, great_far, low_first, low, low_last))
    less_out = last_step(me, cols_less, less_far, low_first, low, low_last)
    less_out = return_pieces(less_out)
    less, _, minus = later_step(less, cols_great, low, width)
    great, _, last = later_step(great, cols_less, low, width, minus)
    args = (left, unit, later, unit_last, last)
    estimate = pl.CostEstimate(flops=500_000_000, bytes_accessed=1_000_000, transcendentals=0)
    rho = call(finish_kernel, [(density.shape, jnp.float32)], args, estimate)[0]
    rho = whole_total(part_total(rho), density.shape)
    less_row_out = row_step(less, low_last, width).reshape(less_row.shape)
    great_row_out = row_step(great, low_last, width).reshape(great_row.shape)
    return (less_row_out, less_out, great_row_out, great_out, rho)


def solution(mesh):
    history = P(None, None, "col", "hist")
    return jax.shard_map(
        per_device,
        mesh=mesh,
        in_specs=(history, history, history, history, P(), P()),
        out_specs=(history, history, history, history, P()),
        check_vma=False,
    )
```

```python
import functools

import jax
import jax.numpy as jnp
from jax import lax
from jax.experimental import pallas as pl
from jax.experimental.pallas import tpu as pltpu
from jax.sharding import PartitionSpec as P


step_length = 0.1
mean_field = 2.0
coupling = 1.0

HIGH = lax.Precision.HIGHEST
SUBLANES = 8
GROUP = 8
SPAN = 256


def dot_high(a, b):
    return jnp.dot(a, b, precision=HIGH, preferred_element_type=jnp.float32)


def eye_mask(size):
    rows = lax.broadcasted_iota(jnp.int32, (size, size), 0)
    return rows == lax.broadcasted_iota(jnp.int32, (size, size), 1)


def inverse(matrix):
    size = matrix.shape[0]
    blocks = [matrix[p : p + SUBLANES] for p in range(0, size, SUBLANES)]
    rows = lax.broadcasted_iota(jnp.int32, (SUBLANES, size), 0)
    lanes = lax.broadcasted_iota(jnp.int32, (SUBLANES, size), 1)
    for p in range(len(blocks)):
        first = p * SUBLANES
        pivot_lanes = (lanes >= first) & (lanes < first + SUBLANES)

        def columns(block):
            return [jnp.broadcast_to(block[:, first + c : first + c + 1], (SUBLANES, size)) for c in range(SUBLANES)]

        pivot = columns(blocks[p])
        row_block = jnp.where(pivot_lanes, jnp.where(lanes == rows + first, 1.0, 0.0), blocks[p])
        for j in range(SUBLANES):

            def across(value):
                return jnp.broadcast_to(value[j : j + 1], (SUBLANES, size))

            scale = 1.0 / across(pivot[j])
            factor = pivot[j]

            def eliminate(value):
                top = across(value) * scale
                return jnp.where(rows == j, top, value - factor * top)

            row_block = eliminate(row_block)
            pivot = [eliminate(value) if c > j else value for c, value in enumerate(pivot)]
        spread = [jnp.broadcast_to(row_block[c : c + 1], (SUBLANES, size)) for c in range(SUBLANES)]
        order = list(range(p + 1, len(blocks))) + list(range(p))
        for q in order:
            total = jnp.where(pivot_lanes, 0.0, blocks[q])
            for c, column in enumerate(columns(blocks[q])):
                total = total - column * spread[c]
            blocks[q] = total
        blocks[p] = row_block
    return jnp.concatenate(blocks, axis=0)


def spread_rows(ref, row):
    ref[...] = jnp.broadcast_to(row.reshape(1, 1, row.shape[-1]), ref.shape)


def diagonal_row(matrix):
    return jnp.sum(jnp.where(eye_mask(matrix.shape[0]), matrix, 0.0), axis=0, keepdims=True)


def solve_kernel(rotates, levels_ref, ham_ref, *refs):
    size = ham_ref.shape[0]
    eye = eye_mask(size)
    level = levels_ref[0]
    for row in range(1, levels_ref.shape[0]):
        level = level + levels_ref[row]
    halved = (0.5 * step_length) * (ham_ref[...] + mean_field * jnp.where(eye, level, 0.0))
    identity = jnp.where(eye, 1.0, 0.0)
    solved = inverse(identity + dot_high(halved, halved))
    unit_real = 2.0 * solved - identity
    unit_imag = -2.0 * dot_high(solved, halved)
    low_real, low_imag = unit_real.astype(jnp.bfloat16), unit_imag.astype(jnp.bfloat16)
    if rotates:
        rho_ref, later_ref, low_ref, unit_ref, left_ref, next_ref = refs
    else:
        low_ref, unit_ref = refs
    low_ref[0:size, 0:size] = low_real
    low_ref[0:size, size:] = low_imag
    low_ref[size:, 0:size] = -low_imag
    low_ref[size:, size:] = low_real
    unit_ref[0] = unit_real
    unit_ref[1] = unit_imag
    if rotates:
        rho_real, rho_imag = rho_ref[0], rho_ref[1]
        left_real = dot_high(unit_real, rho_real) - dot_high(unit_imag, rho_imag)
        left_imag = dot_high(unit_real, rho_imag) + dot_high(unit_imag, rho_real)
        left_ref[0] = left_real
        left_ref[1] = left_imag
        real_diagonal = jnp.sum(left_real * unit_real + left_imag * unit_imag, axis=1, keepdims=True)
        row = jnp.sum(jnp.where(eye, real_diagonal + later_ref[0], 0.0), axis=0, keepdims=True)
        spread_rows(next_ref, row)


IN_VMEM = pl.BlockSpec(memory_space=pltpu.VMEM)
IN_HBM = pl.BlockSpec(memory_space=pl.ANY)


def call(body, outs, args, cost_estimate, scratch=(), scalars=0, streamed=(), streamed_outs=(), grant=8):
    specs = [pl.BlockSpec(memory_space=pltpu.SMEM)] * scalars
    specs += [IN_HBM if i in streamed else IN_VMEM for i in range(scalars, len(args))]
    return pl.pallas_call(
        body,
        out_shape=[
            pltpu.HBM(shape, kind) if i in streamed_outs else jax.ShapeDtypeStruct(shape, kind)
            for i, (shape, kind) in enumerate(outs)
        ],
        in_specs=specs,
        out_specs=[IN_HBM if i in streamed_outs else IN_VMEM for i in range(len(outs))],
        scratch_shapes=list(scratch),
        cost_estimate=cost_estimate,
        compiler_params=pltpu.CompilerParams(vmem_limit_bytes=grant * 2**20 if grant else None),
    )(*args)


def stream(outside, inside, semaphores, base, group, width, inward):
    lanes = lanes_of(base, 0, width)
    ends = (outside.at[:, lanes], inside.at[:, lanes])
    source, target = ends if inward else ends[::-1]
    return pltpu.make_async_copy(source, target, semaphores.at[group])


def solve(levels, hamiltonian, rho=None, later=None):
    size = hamiltonian.shape[0]
    outs = [((2 * size, 2 * size), jnp.bfloat16), ((2, size, size), jnp.float32)]
    args = (levels, hamiltonian)
    if rho is not None:
        outs += [((2, size, size), jnp.float32), (levels.shape, jnp.float32)]
        args += (rho, later)
    estimate = pl.CostEstimate(flops=4_000_000_000, bytes_accessed=1_000_000, transcendentals=0)
    return call(functools.partial(solve_kernel, rho is not None), outs, args, estimate)


def lanes_of(base, first, span):
    return pl.ds(pl.multiple_of(base + first, 128), span)


def sigma_into(sig_ref, row_ref, col_ref, base, rows, span):
    size = sig_ref.shape[0] // 2
    for start in range(0, size, rows):
        for first in range(0, sig_ref.shape[1], span):
            real, imag = pl.ds(start, rows), pl.ds(size + start, rows)
            lanes, here = lanes_of(base, first, span), pl.ds(first, span)
            green_real = row_ref[real, lanes].astype(jnp.float32)
            green_imag = row_ref[imag, lanes].astype(jnp.float32)
            other_real = col_ref[real, lanes].astype(jnp.float32)
            other_imag = col_ref[imag, lanes].astype(jnp.float32)
            square_real = (coupling * coupling) * (green_real * green_real - green_imag * green_imag)
            square_imag = (coupling * coupling * 2.0) * green_real * green_imag
            sig_ref[real, here] = (square_real * other_real - square_imag * other_imag).astype(jnp.bfloat16)
            sig_ref[imag, here] = (square_real * other_imag + square_imag * other_real).astype(jnp.bfloat16)


def overlap(sig, col):
    return lax.dot_general(sig, col, (((1,), (1,)), ((), ())), preferred_element_type=jnp.float32)


def advance_into(out_ref, low, source_ref, base, width, local=False):
    span = min(SPAN, width)
    for first in range(0, width, span):
        lanes = lanes_of(base, first, span)
        target = pl.ds(first, span) if local else lanes
        moved = jnp.dot(low, source_ref[:, lanes], preferred_element_type=jnp.float32)
        out_ref[:, target] = moved.astype(out_ref.dtype)


def row_form(low):
    size = low.shape[0] // 2
    top = jnp.concatenate([low[:size, :size], low[size:, :size]], axis=1)
    bottom = jnp.concatenate([low[:size, size:], low[:size, :size]], axis=1)
    return jnp.concatenate([top, bottom], axis=0)


def each_group(total_width, width, body):
    def step(g, carry):
        body(pl.multiple_of(g * width, width), g)
        return carry

    lax.fori_loop(0, total_width // width, step, 0)


def complex_sum(four):
    size = four.shape[0] // 2
    return four[:size, :size] - four[size:, size:], four[:size, size:] + four[size:, :size]


def finish_sum(acc, before_ref, base_ref, out_ref, scale):
    real, imag = complex_sum(scale * (acc[...] - before_ref[...]))
    if base_ref is not None:
        real, imag = base_ref[0] + real, base_ref[1] + imag
    out_ref[0] = real
    out_ref[1] = imag
    return real


def now_kernel(parts, last, me_ref, row_hbm, *refs):
    pieces, refs = refs[:parts], refs[parts:]
    if last:
        before_ref, known_ref, col_hbm, rho_out, level_out, acc, *refs = refs
    else:
        col_hbm, acc, *refs = refs
    sig, place, col_out, row_ref, held, sent, row_came, came = refs
    _, _, _, block, times = held.shape
    total_width, width = col_out.shape[1], sig.shape[1]
    group = width // times
    size = sig.shape[0] // 2
    direct = place.dtype == col_out.dtype
    arrivals = [pltpu.make_async_copy(pieces[r], held.at[r], came.at[r]) for r in range(parts)]
    for copy in arrivals:
        copy.start()
    each_group(total_width, width, lambda base, g: stream(row_hbm, row_ref, row_came, base, g, width, True).start())
    acc[...] = jnp.zeros_like(acc)
    for copy in arrivals:
        copy.wait()

    def body(base, g):
        first = lax.div(base, times)
        for r in range(parts):
            source = lax.bitwise_xor(me_ref[0], r) * block
            for part in range(2):
                rows = pl.ds(pl.multiple_of(part * size + source, block), block)
                for k in range(group):
                    value = held[r, part, first + k]
                    if direct:
                        col_out[rows, lanes_of(base, k * times, times)] = value
                    else:
                        place[rows, pl.ds(k * times, times)] = value.astype(place.dtype)
        if not direct:
            col_out[:, lanes_of(base, 0, width)] = place[...].astype(col_out.dtype)
        stream(col_hbm, col_out, sent, base, g, width, False).start()
        stream(row_hbm, row_ref, row_came, base, g, width, True).wait()
        sigma_into(sig, row_ref, col_out, base, 16, min(SPAN, width))
        acc[...] += overlap(sig[...], col_out[:, lanes_of(base, 0, width)])

    each_group(total_width, width, body)
    if last:
        real = finish_sum(acc, before_ref, known_ref, rho_out, step_length)
        spread_rows(level_out, diagonal_row(real))
    each_group(total_width, width, lambda base, g: stream(col_hbm, col_out, sent, base, g, width, False).wait())


def later_kernel(last, row_hbm, col_hbm, low_ref, *refs):
    if last:
        before_ref, row_to, col_to, sum_out, acc, *refs = refs
    else:
        row_to, col_to, acc, *refs = refs
    sig, row_ref, col_ref, row_out, col_out, row_came, col_came, row_went, col_went = refs
    total_width, width = row_ref.shape[1], sig.shape[1]

    def loads(base, g):
        return (
            stream(row_hbm, row_ref, row_came, base, g, width, True),
            stream(col_hbm, col_ref, col_came, base, g, width, True),
        )

    def stores(base, g):
        return (
            stream(row_to, row_out, row_went, base, g, width, False),
            stream(col_to, col_out, col_went, base, g, width, False),
        )

    def start(base, g):
        for copy in loads(base, g):
            copy.start()

    def wait(base, g):
        for copy in stores(base, g):
            copy.wait()

    each_group(total_width, width, start)
    acc[...] = jnp.zeros_like(acc)

    def body(base, g):
        for copy in loads(base, g):
            copy.wait()
        advance_into(row_out, row_form(low_ref[...]), row_ref, base, width)
        advance_into(col_out, low_ref[...], col_ref, base, width)
        for copy in stores(base, g):
            copy.start()
        sigma_into(sig, row_out, col_out, base, 16, min(SPAN, width))
        acc[...] += overlap(sig[...], col_out[:, lanes_of(base, 0, width)])

    each_group(total_width, width, body)
    if last:
        finish_sum(acc, before_ref, None, sum_out, step_length)
    each_group(total_width, width, wait)


def finish_kernel(left_ref, unit_ref, later_ref, unit_last_ref, last_ref, rho_ref):
    def right(real, imag, unit):
        turned_real, turned_imag = unit[0].T, unit[1].T
        return (
            dot_high(real, turned_real) + dot_high(imag, turned_imag),
            dot_high(imag, turned_real) - dot_high(real, turned_imag),
        )

    real, imag = right(left_ref[0], left_ref[1], unit_ref)
    real, imag = real + later_ref[0], imag + later_ref[1]
    unit_real, unit_imag = unit_last_ref[0], unit_last_ref[1]
    left_real = dot_high(unit_real, real) - dot_high(unit_imag, imag)
    left_imag = dot_high(unit_real, imag) + dot_high(unit_imag, real)
    real, imag = right(left_real, left_imag, unit_last_ref)
    rho_ref[0] = real + last_ref[0]
    rho_ref[1] = imag + last_ref[1]


def row_kernel(width, row_ref, low_ref, row_out):
    low = row_form(low_ref[...])
    each_group(row_ref.shape[1], width, lambda base, g: advance_into(row_out, low, row_ref, base, width))


def last_kernel(parts, me_ref, col_ref, low_first_ref, low_ref, low_last_ref, *refs):
    pieces, outs, (place, once, moved) = refs[:parts], refs[parts : 2 * parts], refs[2 * parts :]
    _, mirrored, block, times = pieces[0].shape
    size, width = moved.shape[0] // 2, moved.shape[1]
    count = col_ref.shape[1] // times

    def advance(out_ref, low, source_ref, base):
        span = min(SPAN, width)
        for first in range(0, width, span):
            source = source_ref[:, lanes_of(base, first, span)].astype(jnp.bfloat16)
            after = jnp.dot(low[...], source, preferred_element_type=jnp.float32)
            out_ref[:, pl.ds(first, span)] = after.astype(jnp.bfloat16).astype(out_ref.dtype)

    def cut(r, to):
        target = lax.bitwise_xor(me_ref[0], r) * block
        for part in range(2):
            rows = pl.ds(pl.multiple_of(part * size + target, block), block)
            for k in range(mirrored):
                outs[r][part, to + k] = moved[rows, pl.ds(k * times, times)].astype(outs[r].dtype)

    def body(base, g):
        first = lax.div(base, times)
        advance(once, low_ref, col_ref, base)
        advance(moved, low_last_ref, once, 0)
        for r in range(parts // 2):
            cut(r, first)

        @pl.when(first >= mirrored)
        def _():
            for r in range(parts // 2, parts):
                cut(r, first - mirrored)

    each_group(count * times, width, body)
    for r in range(parts):
        source = lax.bitwise_xor(me_ref[0], r) * block
        for part in range(2):
            rows = pl.ds(pl.multiple_of(part * size + source, block), block)
            for k in range(mirrored):
                place[rows, pl.ds(k * times, times)] = pieces[r][part, k].astype(place.dtype)
    advance(once, low_first_ref, place, 0)
    advance(place, low_ref, once, 0)
    advance(moved, low_last_ref, place, 0)
    for r in range(parts // 2):
        cut(r, count)


def cost(arrays, products):
    return pl.CostEstimate(flops=products * 2 * 256 * 256 * 4096, bytes_accessed=arrays * 2**21, transcendentals=0)


def place_type(block):
    return jnp.bfloat16 if block % 16 == 0 else jnp.float32


def sum_scratch(size, width):
    return [pltpu.VMEM((2 * size, 2 * size), jnp.float32), pltpu.VMEM((2 * size, width), jnp.bfloat16)]


def now_step(me, row, pieces, before=None, known=None, devices=0):
    parts = len(pieces)
    _, count, block, times = pieces[0].shape
    size = parts * block
    width = min(GROUP, count) * times
    groups = row.shape[1] // width
    square, history = ((2 * size, 2 * size), jnp.float32), (row.shape, jnp.bfloat16)
    args = (me, row, *pieces)
    scratch = sum_scratch(size, width)
    scratch += [pltpu.VMEM((2 * size, width), place_type(block))] + [pltpu.VMEM(row.shape, jnp.bfloat16)] * 2
    scratch += [pltpu.VMEM((parts,) + pieces[0].shape, jnp.bfloat16)]
    scratch += [pltpu.SemaphoreType.DMA((groups,))] * 2 + [pltpu.SemaphoreType.DMA((parts,))]
    body = functools.partial(now_kernel, parts, before is not None)
    if before is None:
        outs, scratch = [history, square], scratch[1:]
    else:
        outs, args = [history, ((2, size, size), jnp.float32), ((devices, 1, size), jnp.float32)], args + (before, known)
    return call(body, outs, args, cost(4, 2), scratch, 1, range(1, parts + 2), (0,), None)


def later_step(row, col, low, width, before=None):
    double = row.shape[0]
    square, history = ((double, double), jnp.float32), (row.shape, jnp.bfloat16)
    body = functools.partial(later_kernel, before is not None)
    scratch = sum_scratch(double // 2, width) + [pltpu.VMEM(row.shape, jnp.bfloat16)] * 4
    scratch += [pltpu.SemaphoreType.DMA((row.shape[1] // width,))] * 4
    if before is None:
        outs, args, scratch = [history, history, square], (row, col, low), scratch[1:]
    else:
        outs, args = [history, history, ((2, double // 2, double // 2), jnp.float32)], (row, col, low, before)
    return call(body, outs, args, cost(4, 3), scratch, 0, (0, 1), (0, 1), None)


def row_step(row, low, width):
    body = functools.partial(row_kernel, width)
    return call(body, [(row.shape, jnp.bfloat16)], (row, low), cost(2, 1))[0]


def last_step(me, col, pieces, low_first, low, low_last):
    double, parts = col.shape[0], len(pieces)
    _, mirrored, block, times = pieces[0].shape
    count = col.shape[1] // times
    near = ((2, count + mirrored, block, times), jnp.bfloat16)
    far = ((2, count - mirrored, block, times), jnp.bfloat16)
    outs = [near] * (parts // 2) + [far] * (parts - parts // 2)
    kind = place_type(block)
    scratch = [pltpu.VMEM((double, mirrored * times), k) for k in (kind, jnp.bfloat16, kind)]
    body = functools.partial(last_kernel, parts)
    return call(body, outs, (me, col, low_first, low, low_last, *pieces), cost(3, 2), scratch, 1)


def tree_sum(values):
    while len(values) > 1:
        values = [values[i] + values[i + 1] for i in range(0, len(values), 2)]
    return values[0]


def swap(value, name, r):
    return lax.ppermute(value, name, [(j, j ^ r) for j in range(lax.axis_size(name))])


def part_total(values):
    count = lax.axis_size("hist")
    rows = values.reshape(count, -1, values.shape[-1])
    share = jnp.sum(lax.all_to_all(rows, "hist", 0, 0, tiled=True), axis=0)
    return share


def whole_total(share, shape):
    count = lax.axis_size("hist")
    moved = [share]
    for r in range(1, lax.axis_size("col")):
        moved.append(swap(share, "col", r))
    share = tree_sum(moved)
    return lax.all_to_all(jnp.broadcast_to(share, (count,) + share.shape), "hist", 0, 0, tiled=True).reshape(shape)


def finish_rotation(left, unit):
    high = functools.partial(jnp.dot, precision=HIGH)
    real = high(left[0], unit[0].T) + high(left[1], unit[1].T)
    imag = high(left[1], unit[0].T) - high(left[0], unit[1].T)
    return jnp.stack([real, imag])


def rotate(unit, rho):
    high = functools.partial(jnp.dot, precision=HIGH)
    real = high(unit[0], rho[0]) - high(unit[1], rho[1])
    imag = high(unit[0], rho[1]) + high(unit[1], rho[0])
    return finish_rotation((real, imag), unit)


def gather_pieces(col):
    me, parts = lax.axis_index("col"), lax.axis_size("col")
    count = col.shape[1] // parts
    pieces = []
    for r in range(parts):
        piece = lax.dynamic_slice_in_dim(col, (me ^ r) * count, count, axis=1)
        pieces.append(swap(piece, "col", r) if r else piece)
    return pieces


def mirror_slices(col, mirrored):
    me, parts = lax.axis_index("col"), lax.axis_size("col")
    count = col.shape[1] // parts
    starts = [(me ^ r ^ (parts // 2)) * count for r in range(parts)]
    return [lax.dynamic_slice_in_dim(col, start, mirrored, axis=1) for start in starts]


def mirror_pieces(slices):
    pieces = []
    for r, piece in enumerate(slices):
        pieces.append(swap(piece, "col", r) if r else piece)
    return pieces


def return_pieces(pieces):
    me, parts = lax.axis_index("col"), lax.axis_size("col")
    _, near, block, times = pieces[0].shape
    mirrored = (near - pieces[-1].shape[1]) // 2
    count = near - mirrored
    out = jnp.zeros((2, parts * count, block, times), pieces[0].dtype)
    half = parts // 2
    for r in [half, 0] + [r for r in range(1, parts) if r != half]:
        moved = pieces[r] if r == 0 else swap(pieces[r], "col", r)
        if r < half:
            out = lax.dynamic_update_slice_in_dim(out, moved[:, :count], (me ^ r) * count, axis=1)
            out = lax.dynamic_update_slice_in_dim(out, moved[:, count:], (me ^ r ^ half) * count, axis=1)
        else:
            out = lax.dynamic_update_slice_in_dim(out, moved, (me ^ r) * count + mirrored, axis=1)
    return out


def per_device(less_row, less_col, great_row, great_col, density, hamiltonian):
    size, count, times = less_row.shape[1:]
    parts = lax.axis_size("col")
    devices = parts * lax.axis_size("hist")
    me = lax.axis_index("col").astype(jnp.int32).reshape(1)
    width = min(GROUP, count) * times
    mirrored = count // 4

    great_pieces = gather_pieces(great_col)
    less_pieces = gather_pieces(less_col)
    great_slices = mirror_slices(great_col, mirrored)
    less_slices = mirror_slices(less_col, mirrored)

    symmetric = 0.5 * (hamiltonian + hamiltonian.T)
    low_first, unit = solve(diagonal_row(density[0]).reshape(1, 1, size), symmetric)
    known = rotate(unit, density * (1.0 / devices))

    less = less_row.reshape(2 * size, count * times)
    great = great_row.reshape(2 * size, count * times)
    cols_great, minus = now_step(me, less, great_pieces)
    less, cols_great, minus_later = later_step(less, cols_great, low_first, width)
    less_pieces, minus_later = lax.optimization_barrier((less_pieces, minus_later))
    cols_less, rho, part = now_step(me, great, less_pieces, minus, known, devices)

    levels = lax.all_to_all(part, ("hist", "col"), 0, 0, tiled=True)
    great_slices, _ = lax.optimization_barrier((great_slices, part))
    great_far = mirror_pieces(great_slices)
    great, cols_less, later = later_step(great, cols_less, low_first, width, minus_later)
    low, unit, left, part = solve(levels, symmetric, rho, later)

    levels = lax.all_to_all(part, ("hist", "col"), 0, 0, tiled=True)
    less_slices, _ = lax.optimization_barrier((less_slices, part))
    less_far = mirror_pieces(less_slices)
    low_last, unit_last = solve(levels, symmetric)

    great_out = return_pieces(last_step(me, cols_great, great_far, low_first, low, low_last))
    less_out = last_step(me, cols_less, less_far, low_first, low, low_last)
    less_out = return_pieces(less_out)
    less, _, minus = later_step(less, cols_great, low, width)
    great, _, last = later_step(great, cols_less, low, width, minus)
    args = (left, unit, later, unit_last, last)
    estimate = pl.CostEstimate(flops=500_000_000, bytes_accessed=1_000_000, transcendentals=0)
    rho = call(finish_kernel, [(density.shape, jnp.float32)], args, estimate)[0]
    rho = whole_total(part_total(rho), density.shape)
    less_row_out = row_step(less, low_last, width).reshape(less_row.shape)
    great_row_out = row_step(great, low_last, width).reshape(great_row.shape)
    return (less_row_out, less_out, great_row_out, great_out, rho)


def solution(mesh):
    history = P(None, None, "col", "hist")
    return jax.shard_map(
        per_device,
        mesh=mesh,
        in_specs=(history, history, history, history, P(), P()),
        out_specs=(history, history, history, history, P()),
        check_vma=False,
    )
```
